32 devices in a mesh: curve: 8 (over z, x), level: 4 (over y, core).
Axes of the slice: x: 2, y: 2, z: 4, core: 2. Of those that a mesh axis runs over, the one named last changes fastest.
Arguments:
- right_side: float32 [512, 4096], P(None, ('curve', 'level')), may hold values from -6 to 6
- counts: int32 [32], replicated, may hold values from 96 to 128, as said below
- neighbours: int32 [6, 4096], P(None, ('curve', 'level')), may hold values from -1 to 4095, as said below
Outputs:
- solution: float32 [512, 4096], P(None, ('curve', 'level'))
- residual: float32 [512, 4096], P(None, ('curve', 'level'))
- residual_norm: float32 [], replicated
The draws below stay inside these ranges and needn't reach their ends.
Inputs may be any that keep to these rules, and one draw needn't show every extreme that they name: `counts`: some device holds 128 live bricks and some device holds 96. `neighbours`: A slot's global number is its device times 128 plus its position. The relation is symmetric across opposite faces; padding slots have -1 on every face and no brick names them. Live bricks are numbered along the curve; the brick across face 0, 2 or 4 lies earlier on the curve and the one across face 1, 3 or 5 later, at most 256 live bricks away.
All inputs are finite; a program needn't handle non-finite values.
Results may differ from the reference program's by a relative error of at most 0.00027.
Values sent between devices are 32-bit elements; how exact they have to be, the bound alone decides.
A program may use at most 64 MiB of HBM per device.

```python
import jax
import jax.numpy as jnp
from jax import lax

SLOT_DEV = 128
MIN_LIVE = 96
SIDE = 16
LAYER = 256
CELLS = 512
SLOTS = 4096


def brick_layout(key):
    device_total = SLOTS // SLOT_DEV
    counts = jax.random.randint(jax.random.fold_in(key, 11), (device_total,), MIN_LIVE, SLOT_DEV + 1)
    fullest = jax.random.randint(jax.random.fold_in(key, 12), (), 0, device_total)
    emptiest = (fullest + 1 + jax.random.randint(jax.random.fold_in(key, 13), (), 0, device_total - 1)) % device_total
    device_ids = jnp.arange(device_total)
    counts = jnp.where(device_ids == fullest, SLOT_DEV, counts)
    counts = jnp.where(device_ids == emptiest, MIN_LIVE, counts)
    return counts.astype(jnp.int32)


def morton_split(morton):
    coord_x = jnp.zeros_like(morton)
    coord_y = jnp.zeros_like(morton)
    for bit_index in range(8):
        coord_x = coord_x | (morton >> 2 * bit_index & 1) << bit_index
        coord_y = coord_y | (morton >> 2 * bit_index + 1 & 1) << bit_index
    return (coord_x, coord_y)


def morton_join(coord_x, coord_y):
    morton = jnp.zeros_like(coord_x)
    for bit_index in range(8):
        morton = morton | (coord_x >> bit_index & 1) << 2 * bit_index
        morton = morton | (coord_y >> bit_index & 1) << 2 * bit_index + 1
    return morton


def draw_counts(key, part):
    return brick_layout(key)


def draw_neighbours(key, part):
    counts = brick_layout(key)
    starts = (jnp.cumsum(counts) - counts).astype(jnp.int32)
    total_live = jnp.sum(counts).astype(jnp.int32)
    slot_ids = jnp.arange(SLOTS, dtype=jnp.int32)
    device_of = slot_ids // SLOT_DEV
    offset = slot_ids % SLOT_DEV
    live_slot = offset < counts[device_of]
    live_index = starts[device_of] + offset
    layer_index = live_index // LAYER
    coord_x, coord_y = morton_split(live_index % LAYER)
    columns = []
    for step_x, step_y, step_z in [(-1, 0, 0), (1, 0, 0), (0, -1, 0), (0, 1, 0), (0, 0, -1), (0, 0, 1)]:
        next_x = coord_x + step_x
        next_y = coord_y + step_y
        next_z = layer_index + step_z
        inside = (next_x >= 0) & (next_x < SIDE) & (next_y >= 0) & (next_y < SIDE) & (next_z >= 0)
        other = next_z * LAYER + morton_join(jnp.clip(next_x, 0, SIDE - 1), jnp.clip(next_y, 0, SIDE - 1))
        inside = inside & (other < total_live) & live_slot
        other = jnp.clip(other, 0, total_live - 1)
        owner = (jnp.searchsorted(starts, other, side='right') - 1).astype(jnp.int32)
        global_slot = owner * SLOT_DEV + other - starts[owner]
        columns.append(jnp.where(inside, global_slot, -1))
    return jnp.stack(columns).astype(jnp.int32)


def shard_levels(key, shape, split, least, high):
    loudness = 1.0
    for axis_at, shards_of in split:
        draws = jax.random.uniform(jax.random.fold_in(jax.random.fold_in(key, 6), axis_at), (shards_of,), jnp.float32, least / len(split), high / len(split))
        loudness = loudness * jnp.repeat(jnp.exp(draws), shape[axis_at] // shards_of).reshape((-1,) + (1,) * (len(shape) - 1 - axis_at))
    return loudness


def bell_draw(stream_key, dims, width, limit, pieces=(), kind=jnp.bfloat16):
    drawn = width * jax.random.normal(stream_key, dims, jnp.float32)
    if pieces:
        drawn = drawn * shard_levels(stream_key, dims, pieces, -0.22, 0.18)
    return jnp.clip(drawn, -limit, limit).astype(kind)


def setup_inputs(seed: int = 0) -> dict:
    arg_keys = jax.random.split(jax.random.key(seed), 4)
    right_side = bell_draw(arg_keys[0], (CELLS, SLOTS), 1.0, 6.0, ((1, 32),), jnp.float32)
    counts = draw_counts(jax.random.fold_in(arg_keys[3], 71), 0)
    neighbours = draw_neighbours(jax.random.fold_in(arg_keys[3], 71), 0)
    return {"right_side": right_side, "counts": counts, "neighbours": neighbours}


OPPOSITE = (1, 0, 3, 2, 5, 4)
RELAXATION = 2.0 / 3.0

def brick_faces(values, extent):
    volume = values.reshape(extent, extent, extent, -1)
    surfaces = [volume[0], volume[extent - 1], volume[:, 0], volume[:, extent - 1], volume[:, :, 0], volume[:, :, extent - 1]]
    return jnp.stack([one_face.reshape(extent * extent, -1) for one_face in surfaces])

def gather_ghosts(lookup, position, present):
    ghosts = []
    for face_id in range(6):
        picked = jnp.take(lookup[OPPOSITE[face_id]], position[face_id], axis=1)
        ghosts.append(jnp.where(present[face_id][None, :], picked, jnp.zeros_like(picked)))
    return ghosts

def apply_operator(values, ghosts, extent, weight):
    brick_count = values.shape[1]
    volume = values.reshape(extent, extent, extent, brick_count)
    padded = jnp.pad(volume, ((1, 1), (1, 1), (1, 1), (0, 0)))
    shaped = [ghost.reshape(extent, extent, brick_count) for ghost in ghosts]
    padded = padded.at[0, 1:-1, 1:-1].set(shaped[0])
    padded = padded.at[-1, 1:-1, 1:-1].set(shaped[1])
    padded = padded.at[1:-1, 0, 1:-1].set(shaped[2])
    padded = padded.at[1:-1, -1, 1:-1].set(shaped[3])
    padded = padded.at[1:-1, 1:-1, 0].set(shaped[4])
    padded = padded.at[1:-1, 1:-1, -1].set(shaped[5])
    beside = padded[2:, 1:-1, 1:-1] + padded[:-2, 1:-1, 1:-1]
    beside = beside + padded[1:-1, 2:, 1:-1] + padded[1:-1, :-2, 1:-1]
    beside = beside + padded[1:-1, 1:-1, 2:] + padded[1:-1, 1:-1, :-2]
    return ((6.0 * volume - beside) * weight).reshape(extent * extent * extent, brick_count)

def restrict(values):
    brick_count = values.shape[1]
    grouped = values.reshape(4, 2, 4, 2, 4, 2, brick_count)
    return lax.optimization_barrier(jnp.mean(grouped, axis=(1, 3, 5))).reshape(64, brick_count)

def prolong(coarse):
    brick_count = coarse.shape[1]
    spread = jnp.broadcast_to(coarse.reshape(4, 1, 4, 1, 4, 1, brick_count), (4, 2, 4, 2, 4, 2, brick_count))
    return spread.reshape(512, brick_count)

def precondition(residual_in, exchange):
    relax_fine = RELAXATION / 6.0
    relax_coarse = RELAXATION / 1.5
    sweep_one = relax_fine * residual_in
    sweep_two = sweep_one + relax_fine * (residual_in - apply_operator(sweep_one, exchange(brick_faces(sweep_one, 8)), 8, 1.0))
    defect = residual_in - apply_operator(sweep_two, exchange(brick_faces(sweep_two, 8)), 8, 1.0)
    coarse_rhs = restrict(defect)
    coarse_one = relax_coarse * coarse_rhs
    coarse_two = coarse_one + relax_coarse * (coarse_rhs - apply_operator(coarse_one, exchange(brick_faces(coarse_one, 4)), 4, 0.25))
    sweep_three = sweep_two + prolong(coarse_two)
    return sweep_three + relax_fine * (residual_in - apply_operator(sweep_three, exchange(brick_faces(sweep_three, 8)), 8, 1.0))

def reference(right_side, counts, neighbours):
    slot_ids = jnp.arange(SLOTS, dtype=jnp.int32)
    live_slot = slot_ids % SLOT_DEV < counts[slot_ids // SLOT_DEV]
    residual_in = jnp.where(live_slot[None, :], right_side, jnp.zeros_like(right_side))
    present = neighbours >= 0
    position = jnp.where(present, neighbours, 0).astype(jnp.int32)

    def exchange(surface):
        return gather_ghosts(surface, position, present)
    preconditioned = precondition(residual_in, exchange)
    image = apply_operator(preconditioned, exchange(brick_faces(preconditioned, 8)), 8, 1.0)
    along = jnp.sum(residual_in * preconditioned)
    curvature = jnp.sum(preconditioned * image)
    step_size = along / curvature
    solution = step_size * preconditioned
    residual = residual_in - step_size * image
    residual_norm = jnp.sqrt(jnp.sum(residual * residual))
    return (solution, residual, residual_norm)
```

```python
import functools

import jax
import jax.numpy as jnp
from jax import lax
from jax.experimental import pallas as pl
from jax.experimental.pallas import tpu as pltpu
from jax.sharding import PartitionSpec as P

MIN_LIVE = 96
LAYER = 256
HOPS = 3
PIECES = 2
AXES = ("curve", "level")
MESH = pl.DeviceIdType.MESH
RELAXATION = 2.0 / 3.0
RELAX_FINE = RELAXATION / 6.0
RELAX_COARSE = RELAXATION / 1.5
F32 = jnp.float32


def kernel(
    sizes,
    stages,
    right_ref,
    counts_ref,
    neighbours_ref,
    first,
    image,
    source,
    tile_ref,
    second,
    zghost,
    paired,
    coarse,
    shifted,
    doubled,
    held,
    applied_ref,
    faces_fine,
    packed_fine,
    windows_fine,
    faces_coarse,
    packed_coarse,
    windows_coarse,
    sums,
    *sems,
):
    link_sems, relay_sems, pair_sems, far_sems, (sum_send, sum_recv) = [
        sems[i : i + 2] for i in range(0, 10, 2)
    ]
    curve_size, level_size = sizes
    total = curve_size * level_size
    me = lax.axis_index("curve") * level_size + lax.axis_index("level")
    lanes = right_ref.shape[1]
    half = lanes // 2

    def place(index):
        return (index // level_size, index % level_size)

    barrier = pltpu.get_barrier_semaphore()
    greeted = 0
    for size, _, peer in stages:
        for k in range(1, size):
            pl.semaphore_signal(barrier, inc=1, device_id=peer(k), device_id_type=MESH)
            greeted += 1
    direct = len(stages) == 1
    if not direct:
        for hop in range(1, HOPS + 1):
            for sign in (1, -1):
                target = (me + sign * hop + total) % total
                pl.semaphore_signal(barrier, inc=1, device_id=place(target), device_id_type=MESH)
                greeted += 1

    lane = lax.broadcasted_iota(jnp.int32, (1, lanes), 1)
    own_count = counts_ref[me]
    live = lane < own_count
    for x in range(8):
        rows = pl.ds(64 * x, 64)
        value = jnp.where(live, right_ref[rows, :], 0.0)
        source[rows, :] = value
        first[rows, :] = RELAX_FINE * value

    nb = neighbours_ref[...]
    present = nb >= 0
    owner = nb // lanes
    offset = nb % lanes
    face_id = lax.broadcasted_iota(jnp.int32, nb.shape, 0)
    hop_of = jnp.where(face_id % 2 == 0, me - owner, owner - me)
    hop_of = jnp.where(present, hop_of, -1)
    far_count = counts_ref[jnp.maximum(me - HOPS, 0)]
    odd = me % 2
    even = 1 - odd
    partner = me + 1 - 2 * odd
    earlier_pair = me >= 2
    later_pair = me - odd + 2 < total
    reaches = (1 + 2 * even, 1 + 2 * odd)
    arrives = (2 * odd, 2 * even)
    far_there = jnp.where(odd == 1, me + HOPS < total, me >= HOPS)
    far_device = (me + HOPS * (2 * odd - 1) + total) % total
    skipped = jnp.where(
        (face_id % 2 == 0) & (hop_of == HOPS), even * (far_count - half), 0
    )
    where_at = jnp.clip(offset - skipped, 0, lanes - 1)
    low_half = jnp.broadcast_to(lane < half, (8, lanes))
    pack_index = jnp.broadcast_to(odd * (own_count - half) + lane % half, (8, lanes))

    def pick(block, index):
        return jnp.take_along_axis(block, index, axis=1, mode="promise_in_bounds")

    finishing = []

    def send(src, dst, sems, at, target, sends):
        made = pltpu.make_async_remote_copy(
            src_ref=src,
            dst_ref=dst,
            send_sem=sems[0].at[at],
            recv_sem=sems[1].at[at],
            device_id=place(target),
            device_id_type=MESH,
        )
        finishing.append((made, sends))
        return made

    def exchange(stage, values, extent, faces, packed, windows, meanwhile):
        area = extent * extent
        last = extent - 1
        pack = 3 * area // 2
        for direction in (0, 1):
            at = last if direction == 0 else 0
            faces[direction, 0:area, :] = values[pl.ds(at * area, area), :]
            for x in range(extent):
                faces[direction, pl.ds(area + x * extent, extent), :] = values[
                    pl.ds(x * area + at * extent, extent), :
                ]
            faces[direction, pl.ds(2 * area, area), :] = values[pl.ds(at, area, extent), :]
        if stage == 0:
            pl.semaphore_wait(barrier, greeted)
        links = []
        for chunk in range(3):
            rows = pl.ds(chunk * area, area)
            for direction in (0, 1):
                reach = reaches[direction]
                target = me + reach if direction == 0 else me - reach
                made = send(
                    faces.at[direction, rows],
                    windows.at[direction, reach - 1, rows],
                    link_sems,
                    (stage, direction, chunk),
                    (target + total) % total,
                    later_pair if direction == 0 else earlier_pair,
                )
                pl.when(later_pair if direction == 0 else earlier_pair)(made.start)
                links.append((direction, chunk, rows, made))
        inside = send(faces.at[odd], windows.at[odd, 0], pair_sems, (stage,), partner, None)
        inside.start()
        for r in range(0, pack, 8):
            a = pick(faces[1 - odd, pl.ds(r, 8), :], pack_index)
            b = pick(faces[1 - odd, pl.ds(pack + r, 8), :], pack_index)
            packed[pl.ds(r, 8), :] = jnp.where(low_half, a, b)
        far = send(
            packed, windows.at[1 - odd, 2, pl.ds(0, pack)], far_sems, (stage,), far_device, far_there
        )
        pl.when(far_there)(far.start)
        def ghost(face, hops_in, blocks):
            direction, slot = face % 2, face // 2
            at = jnp.broadcast_to(where_at[face : face + 1, :], (8, lanes))
            is_packed = odd == direction
            at_high = jnp.where(is_packed, jnp.minimum(at + half, lanes - 1), at)
            hops = jnp.broadcast_to(hop_of[face : face + 1, :], (8, lanes))
            pieces = []
            for r in range(0, area, 8):
                row = slot * area + r
                block = blocks[r // 8]
                for hop in hops_in:
                    index = at
                    if hop == 0:
                        window = faces[direction, pl.ds(row, 8), :]
                    elif hop < HOPS or row < pack:
                        window = windows[direction, hop - 1, pl.ds(row, 8), :]
                    else:
                        start = pl.multiple_of(row - jnp.where(is_packed, pack, 0), 8)
                        window = windows[direction, hop - 1, pl.ds(start, 8), :]
                        index = at_high
                    block = jnp.where(hops == hop, pick(window, index), block)
                pieces.append(block)
            return pieces

        empty = [jnp.zeros((8, lanes), F32)] * (area // 8)
        for face in range(6):
            for r, block in enumerate(ghost(face, (0,), empty)):
                held[face, pl.ds(8 * r, 8), :] = block
        meanwhile()
        relays = []
        for direction, chunk, rows, made in links:
            comes = earlier_pair if direction == 0 else later_pair
            relay = send(
                windows.at[direction, arrives[direction], rows],
                windows.at[direction, 1, rows],
                relay_sems,
                (stage, direction, chunk),
                partner,
                comes,
            )

            @pl.when(comes)
            def _():
                made.wait_recv()
                relay.start()

            relays.append((relay, comes))
        inside.wait_recv()
        pl.when(far_there)(far.wait_recv)
        ghosts = []
        for face in range(6):
            relay, comes = relays[face]
            pl.when(comes)(relay.wait_recv)
            blocks = [held[face, pl.ds(r, 8), :] for r in range(0, area, 8)]
            ghosts.append(jnp.concatenate(ghost(face, (1, 2, 3), blocks), axis=0))
        return ghosts

    zrow = lax.broadcasted_iota(jnp.int32, (8, 8, lanes), 1)

    zghost[...] = jnp.zeros_like(zghost)

    def inner(values):
        for x in range(8):
            rows = pl.ds(64 * x, 64)
            here = values[rows, :]
            edge = jnp.zeros((8, lanes), F32)
            beside = jnp.concatenate([edge, here[:-8]], axis=0) + jnp.concatenate(
                [here[8:], edge], axis=0
            )
            if x > 0:
                beside = beside + values[pl.ds(64 * (x - 1), 64), :]
            if x < 7:
                beside = beside + values[pl.ds(64 * (x + 1), 64), :]
            cube = here.reshape(8, 8, lanes)
            below = jnp.where(zrow == 0, 0.0, pltpu.roll(cube, 1, 1))
            above = jnp.where(zrow == 7, 0.0, pltpu.roll(cube, 7, 1))
            beside = beside + (below + above).reshape(64, lanes)
            applied_ref[rows, :] = 6.0 * here - beside

    def fine(values, ghosts, use):
        g0, g1, g2, g3, g4, g5 = ghosts
        zghost[pl.ds(0, 64, 8), :] = g4
        zghost[pl.ds(7, 64, 8), :] = g5
        for x in range(8):
            rows = pl.ds(64 * x, 64)
            applied = applied_ref[rows, :] - zghost[rows, :]
            if x == 0:
                applied = applied - g0
            if x == 7:
                applied = applied - g1
            applied = jnp.concatenate(
                [
                    applied[:8] - g2[8 * x : 8 * x + 8],
                    applied[8:56],
                    applied[56:] - g3[8 * x : 8 * x + 8],
                ],
                axis=0,
            )
            use(x, rows, values[rows, :], applied)

    def exchange_fine(stage, k, values):
        return exchange(
            stage,
            values,
            8,
            faces_fine.at[k],
            packed_fine.at[k],
            windows_fine.at[k],
            lambda: inner(values),
        )

    def exchange_coarse(stage, k, meanwhile):
        return exchange(
            stage,
            coarse,
            4,
            faces_coarse.at[k],
            packed_coarse.at[k],
            windows_coarse.at[k],
            meanwhile,
        )

    def sweep(x, rows, here, applied):
        second[rows, :] = here + RELAX_FINE * (source[rows, :] - applied)

    fine(first, exchange_fine(0, 0, first), sweep)

    slabs = []

    def restrict(x, rows, here, applied):
        slabs.append(source[rows, :] - applied)
        if x % 2 == 1:
            both = slabs[x - 1] + slabs[x]
            for y in range(4):
                paired[pl.ds(32 * (x // 2) + 8 * y, 8), :] = (
                    both[16 * y : 16 * y + 8] + both[16 * y + 8 : 16 * y + 16]
                )

    ghosts = exchange_fine(1, 1, second)
    fine(second, ghosts, restrict)
    coarse_rhs = 0.125 * (paired[pl.ds(0, 64, 2), :] + paired[pl.ds(1, 64, 2), :])
    coarse_one = RELAX_COARSE * coarse_rhs
    coarse[...] = coarse_one
    g0, g1, g2, g3, g4, g5 = exchange_coarse(2, 0, lambda: None)
    beside = jnp.concatenate([g0, coarse_one[:-16]], axis=0) + jnp.concatenate(
        [coarse_one[16:], g1], axis=0
    )
    for k, shift in enumerate((4, 60, 1, 63)):
        shifted[k, :, :] = pltpu.roll(coarse_one, shift, 0)
    for x in range(4):
        shifted[0, pl.ds(16 * x, 4), :] = g2[4 * x : 4 * x + 4]
        shifted[1, pl.ds(16 * x + 12, 4), :] = g3[4 * x : 4 * x + 4]
    for x in range(4):
        for y in range(4):
            at = 16 * x + 4 * y
            shifted[2, pl.ds(at, 1), :] = g4[4 * x + y : 4 * x + y + 1]
            shifted[3, pl.ds(at + 3, 1), :] = g5[4 * x + y : 4 * x + y + 1]
    beside = beside + (shifted[0] + shifted[1]) + (shifted[2] + shifted[3])
    coarse_two = coarse_one + RELAX_COARSE * (coarse_rhs - 0.25 * (6.0 * coarse_one - beside))
    coarse[...] = coarse_two
    paired[pl.ds(0, 64, 2), :] = coarse_two
    paired[pl.ds(1, 64, 2), :] = coarse_two

    def correct():
        for x in range(8):
            for y in range(8):
                rows = pl.ds(64 * x + 8 * y, 8)
                lift = paired[pl.ds(32 * (x // 2) + 8 * (y // 2), 8), :]
                second[rows, :] = second[rows, :] + lift
        inner(second)

    corrections = exchange_coarse(3, 1, correct)
    for face in range(6):
        doubled[face, pl.ds(0, 16, 2), :] = corrections[face]
        doubled[face, pl.ds(1, 16, 2), :] = corrections[face]
        ghosts[face] = ghosts[face] + jnp.concatenate(
            [doubled[face, pl.ds(8 * (a // 2), 8), :] for a in range(8)], axis=0
        )

    def smooth(x, rows, here, applied):
        first[rows, :] = here + RELAX_FINE * (source[rows, :] - applied)

    fine(second, ghosts, smooth)

    parts = [jnp.zeros((8, lanes), F32)] * 5

    def fold(block):
        return jnp.sum(block.reshape(8, 8, lanes), axis=0)

    def finish(x, rows, here, applied):
        image[rows, :] = applied
        r = source[rows, :]
        for k, term in enumerate((r * here, here * applied, r * r, r * applied, applied * applied)):
            parts[k] = parts[k] + fold(term)

    fine(first, exchange_fine(4, 2, first), finish)

    tile = jnp.zeros((1, lanes), F32)
    for k in range(5):
        one = jnp.sum(jnp.sum(parts[k], axis=0, keepdims=True), axis=1, keepdims=True)
        tile = jnp.where(lane == k, one, tile)
    base = 0
    for size, mine, peer in stages:
        sums[base + mine] = tile
        copies = []
        for k in range(1, size):
            made = pltpu.make_async_remote_copy(
                src_ref=sums.at[base + mine],
                dst_ref=sums.at[base + mine],
                send_sem=sum_send.at[base + k],
                recv_sem=sum_recv.at[base + k],
                device_id=peer(k),
                device_id_type=MESH,
            )
            made.start()
            copies.append(made)
        for made in copies:
            made.wait_recv()
        tile = jnp.sum(sums[base : base + size], axis=0)
        for made in copies:
            made.wait_send()
        base += size
    tile_ref[...] = tile
    for made, sends in finishing:
        if sends is None:
            made.wait_send()
        else:
            pl.when(sends)(made.wait_send)


def finish(p_ref, image_ref, source_ref, tile_ref, sol_hbm, res_hbm, norm_ref, sol, res, sems):
    lanes = p_ref.shape[1]
    rows_per = p_ref.shape[0] // PIECES
    lane = lax.broadcasted_iota(jnp.int32, (1, lanes), 1)
    tile = tile_ref[...]
    along, curvature, old_square, cross, image_square = [
        jnp.sum(jnp.where(lane == k, tile, 0.0), axis=1, keepdims=True) for k in range(5)
    ]
    step = along / curvature
    copies = []
    for x in range(PIECES):
        rows = pl.ds(rows_per * x, rows_per)
        sol[rows, :] = step * p_ref[rows, :]
        res[rows, :] = source_ref[rows, :] - step * image_ref[rows, :]
        for k, (here, there) in enumerate(((sol, sol_hbm), (res, res_hbm))):
            made = pltpu.make_async_copy(here.at[rows], there.at[rows], sems.at[k, x])
            made.start()
            copies.append(made)
    square = old_square - 2.0 * step * cross + step * step * image_square
    norm_ref[0] = jnp.sqrt(square)[0, 0]
    for made in copies:
        made.wait()


def local(sizes, right_side, counts, neighbours):
    cells, lanes = right_side.shape
    curve_size, level_size = sizes
    total = curve_size * level_size

    def body(*refs):
        curve, level = lax.axis_index("curve"), lax.axis_index("level")
        if total <= 64:
            me = curve * level_size + level

            def everyone(k):
                other = (me + k) % total
                return (other // level_size, other % level_size)

            stages = [(total, me, everyone)]
        else:
            stages = [
                (level_size, level, lambda k: (curve, (level + k) % level_size)),
                (curve_size, curve, lambda k: ((curve + k) % curve_size, level)),
            ]
        kernel(sizes, stages, *refs)

    sum_rows = total if total <= 64 else curve_size + level_size
    vmem = pl.BlockSpec(memory_space=pltpu.VMEM)
    block = jax.ShapeDtypeStruct((cells, lanes), F32)
    whole = pltpu.VMEM((cells, lanes), F32)
    out = pl.pallas_call(
        body,
        out_shape=(whole, whole, whole, pltpu.VMEM((1, lanes), F32)),
        in_specs=[vmem, pl.BlockSpec(memory_space=pltpu.SMEM), vmem],
        out_specs=(vmem,) * 4,
        scratch_shapes=[
            pltpu.VMEM((cells, lanes), F32),
            pltpu.VMEM((cells, lanes), F32),
            pltpu.VMEM((cells // 4, lanes), F32),
            pltpu.VMEM((cells // 8, lanes), F32),
            pltpu.VMEM((4, cells // 8, lanes), F32),
            pltpu.VMEM((6, 32, lanes), F32),
            pltpu.VMEM((6, 64, lanes), F32),
            pltpu.VMEM((cells, lanes), F32),
            pltpu.VMEM((3, 2, 192, lanes), F32),
            pltpu.VMEM((3, 96, lanes), F32),
            pltpu.VMEM((3, 2, HOPS, 192, lanes), F32),
            pltpu.VMEM((2, 2, 48, lanes), F32),
            pltpu.VMEM((2, 24, lanes), F32),
            pltpu.VMEM((2, 2, HOPS, 48, lanes), F32),
            pltpu.VMEM((sum_rows, 1, lanes), F32),
            pltpu.SemaphoreType.DMA((5, 2, 3)),
            pltpu.SemaphoreType.DMA((5, 2, 3)),
            pltpu.SemaphoreType.DMA((5, 2, 3)),
            pltpu.SemaphoreType.DMA((5, 2, 3)),
            pltpu.SemaphoreType.DMA((5,)),
            pltpu.SemaphoreType.DMA((5,)),
            pltpu.SemaphoreType.DMA((5,)),
            pltpu.SemaphoreType.DMA((5,)),
            pltpu.SemaphoreType.DMA((sum_rows,)),
            pltpu.SemaphoreType.DMA((sum_rows,)),
        ],
        compiler_params=pltpu.CompilerParams(collective_id=0, has_side_effects=True),
    )(right_side, counts, neighbours)
    hbm = pl.BlockSpec(memory_space=pl.ANY)
    out = pl.pallas_call(
        finish,
        out_shape=(block, block, jax.ShapeDtypeStruct((1,), F32)),
        in_specs=[vmem] * 4,
        out_specs=(hbm, hbm, pl.BlockSpec(memory_space=pltpu.SMEM)),
        scratch_shapes=[
            pltpu.VMEM((cells, lanes), F32),
            pltpu.VMEM((cells, lanes), F32),
            pltpu.SemaphoreType.DMA((2, PIECES)),
        ],
    )(*[pltpu.with_memory_space_constraint(a, pltpu.VMEM) for a in out])
    return out[0], out[1], out[2].reshape(())


def solution(mesh):
    sizes = tuple(mesh.shape[name] for name in AXES)
    in_specs = (P(None, AXES), P(), P(None, AXES))
    out_specs = (P(None, AXES), P(None, AXES), P())
    return jax.shard_map(
        functools.partial(local, sizes), mesh=mesh, in_specs=in_specs, out_specs=out_specs, check_vma=False
    )
```

```python
import functools

import jax
import jax.numpy as jnp
from jax import lax
from jax.experimental import pallas as pl
from jax.experimental.pallas import tpu as pltpu
from jax.sharding import PartitionSpec as P

MIN_LIVE = 96
LAYER = 256
HOPS = 3
PIECES = 2
AXES = ("curve", "level")
MESH = pl.DeviceIdType.MESH
RELAXATION = 2.0 / 3.0
RELAX_FINE = RELAXATION / 6.0
RELAX_COARSE = RELAXATION / 1.5
F32 = jnp.float32


def kernel(
    sizes,
    stages,
    right_hbm,
    counts_hbm,
    neighbours_hbm,
    first,
    image,
    source,
    tile_ref,
    counts_ref,
    neighbours_ref,
    second,
    zghost,
    paired,
    halved,
    yghost_coarse,
    zghost_coarse,
    doubled,
    applied_ref,
    ghosts_fine,
    ghosts_coarse,
    faces_fine,
    packed_fine,
    windows_fine,
    faces_coarse,
    packed_coarse,
    windows_coarse,
    sums,
    loads,
    *sems,
):
    link_sems, relay_sems, pair_sems, far_sems, (sum_send, sum_recv) = [
        sems[i : i + 2] for i in range(0, 10, 2)
    ]
    curve_size, level_size = sizes
    total = curve_size * level_size
    me = lax.axis_index("curve") * level_size + lax.axis_index("level")
    lanes = source.shape[1]
    half = lanes // 2

    def place(index):
        return (index // level_size, index % level_size)

    barrier = pltpu.get_barrier_semaphore()
    greeted = 0
    if len(stages) > 1:
        for hop in range(1, HOPS + 1):
            for sign in (1, -1):
                target = (me + sign * hop + total) % total
                pl.semaphore_signal(barrier, inc=1, device_id=place(target), device_id_type=MESH)
                greeted += 1
    for size, _, peer in stages:
        for k in range(1, size):
            pl.semaphore_signal(barrier, inc=1, device_id=peer(k), device_id_type=MESH)
            greeted += 1
    inputs = [
        pltpu.make_async_copy(src, dst, loads.at[k])
        for k, (src, dst) in enumerate(
            ((right_hbm, second), (counts_hbm, counts_ref), (neighbours_hbm, neighbours_ref))
        )
    ]
    for made in inputs:
        made.start()
    zghost[...] = jnp.zeros_like(zghost)
    yghost_coarse[...] = jnp.zeros_like(yghost_coarse)
    zghost_coarse[...] = jnp.zeros_like(zghost_coarse)
    for made in inputs:
        made.wait()

    lane = lax.broadcasted_iota(jnp.int32, (1, lanes), 1)
    own_count = counts_ref[me]
    live = lane < own_count
    for x in range(8):
        rows = pl.ds(64 * x, 64)
        value = jnp.where(live, second[rows, :], 0.0)
        source[rows, :] = value
        first[rows, :] = RELAX_FINE * value

    nb = neighbours_ref[...]
    present = nb >= 0
    owner = nb // lanes
    offset = nb % lanes
    face_id = lax.broadcasted_iota(jnp.int32, nb.shape, 0)
    hop_of = jnp.where(face_id % 2 == 0, me - owner, owner - me)
    hop_of = jnp.where(present, hop_of, -1)
    far_count = counts_ref[jnp.maximum(me - HOPS, 0)]
    odd = me % 2
    even = 1 - odd
    partner = me + 1 - 2 * odd
    earlier_pair = me >= 2
    later_pair = me - odd + 2 < total
    reaches = (1 + 2 * even, 1 + 2 * odd)
    arrives = (2 * odd, 2 * even)
    far_there = jnp.where(odd == 1, me + HOPS < total, me >= HOPS)
    far_device = (me + HOPS * (2 * odd - 1) + total) % total
    skipped = jnp.where(
        (face_id % 2 == 0) & (hop_of == HOPS), even * (far_count - half), 0
    )
    where_at = jnp.clip(offset - skipped, 0, lanes - 1)
    low_half = jnp.broadcast_to(lane < half, (8, lanes))
    pack_index = jnp.broadcast_to(odd * (own_count - half) + lane % half, (8, lanes))

    def pick(block, index):
        return jnp.take_along_axis(block, index, axis=1, mode="promise_in_bounds")

    finishing = []

    def send(src, dst, sems, at, target, sends):
        made = pltpu.make_async_remote_copy(
            src_ref=src,
            dst_ref=dst,
            send_sem=sems[0].at[at],
            recv_sem=sems[1].at[at],
            device_id=place(target),
            device_id_type=MESH,
        )
        finishing.append((made, sends))
        return made

    def cut(values, extent, faces):
        area = extent * extent
        for direction in (0, 1):
            at = extent - 1 if direction == 0 else 0
            faces[direction, 0:area, :] = values[pl.ds(at * area, area), :]
            for x in range(extent):
                faces[direction, pl.ds(area + x * extent, extent), :] = values[
                    pl.ds(x * area + at * extent, extent), :
                ]
            faces[direction, pl.ds(2 * area, area), :] = values[pl.ds(at, area, extent), :]

    class Exchange:
        def __init__(self, stage, area, chunks, faces, packed, windows, ghosts):
            self.stage, self.area, self.chunks = stage, area, chunks
            self.faces, self.packed, self.windows, self.ghosts = faces, packed, windows, ghosts

        def post(self):
            faces, packed, windows, stage = self.faces, self.packed, self.windows, self.stage
            size = 3 * self.area // self.chunks
            pack = 3 * self.area // 2
            self.links = []
            for chunk in range(self.chunks):
                rows = pl.ds(chunk * size, size)
                for direction in (0, 1):
                    reach = reaches[direction]
                    target = me + reach if direction == 0 else me - reach
                    made = send(
                        faces.at[direction, rows],
                        windows.at[direction, reach - 1, rows],
                        link_sems,
                        (stage, direction, chunk),
                        (target + total) % total,
                        later_pair if direction == 0 else earlier_pair,
                    )
                    pl.when(later_pair if direction == 0 else earlier_pair)(made.start)
                    self.links.append((direction, chunk, rows, made))
            self.inside = send(
                faces.at[odd], windows.at[odd, 0], pair_sems, (stage,), partner, None
            )
            self.inside.start()
            for r in range(0, pack, 8):
                a = pick(faces[1 - odd, pl.ds(r, 8), :], pack_index)
                b = pick(faces[1 - odd, pl.ds(pack + r, 8), :], pack_index)
                packed[pl.ds(r, 8), :] = jnp.where(low_half, a, b)
            self.far = send(
                packed,
                windows.at[1 - odd, 2, pl.ds(0, pack)],
                far_sems,
                (stage,),
                far_device,
                far_there,
            )
            pl.when(far_there)(self.far.start)

        def pull(self, face, hops_in):
            area, faces, windows = self.area, self.faces, self.windows
            pack = 3 * area // 2
            direction, slot = face % 2, face // 2
            at = jnp.broadcast_to(where_at[face : face + 1, :], (8, lanes))
            is_packed = odd == direction
            at_high = jnp.where(is_packed, jnp.minimum(at + half, lanes - 1), at)
            hops = jnp.broadcast_to(hop_of[face : face + 1, :], (8, lanes))
            for r in range(0, area, 8):
                row = slot * area + r
                if 0 in hops_in:
                    block = jnp.zeros((8, lanes), F32)
                else:
                    block = self.ghosts[face, pl.ds(r, 8), :]
                for hop in hops_in:
                    index = at
                    if hop == 0:
                        window = faces[direction, pl.ds(row, 8), :]
                    elif hop < HOPS or row < pack:
                        window = windows[direction, hop - 1, pl.ds(row, 8), :]
                    else:
                        start = pl.multiple_of(row - jnp.where(is_packed, pack, 0), 8)
                        window = windows[direction, hop - 1, pl.ds(start, 8), :]
                        index = at_high
                    block = jnp.where(hops == hop, pick(window, index), block)
                self.ghosts[face, pl.ds(r, 8), :] = block

        def near(self):
            for face in range(6):
                self.pull(face, (0,))

        def forward(self):
            self.relays = {}
            for direction, chunk, rows, made in self.links:
                comes = earlier_pair if direction == 0 else later_pair
                relay = send(
                    self.windows.at[direction, arrives[direction], rows],
                    self.windows.at[direction, 1, rows],
                    relay_sems,
                    (self.stage, direction, chunk),
                    partner,
                    comes,
                )

                @pl.when(comes)
                def _():
                    made.wait_recv()
                    relay.start()

                self.relays[direction, chunk] = (relay, comes)

        def collect(self):
            self.inside.wait_recv()
            pl.when(far_there)(self.far.wait_recv)
            for face in range(6):
                waits = self.relays.pop((face % 2, face // 2), None)
                if waits is not None:
                    relay, comes = waits
                    pl.when(comes)(relay.wait_recv)
                self.pull(face, (1, 2, 3))

    def fine_exchange(k):
        return Exchange(
            k, 64, 3, faces_fine.at[k], packed_fine.at[k], windows_fine.at[k], ghosts_fine.at[k]
        )

    def coarse_exchange(k):
        return Exchange(
            3 + k,
            16,
            1,
            faces_coarse.at[k],
            packed_coarse.at[k],
            windows_coarse.at[k],
            ghosts_coarse.at[k],
        )

    zrow = lax.broadcasted_iota(jnp.int32, (8, 8, lanes), 1)

    def inner(values):
        for x in range(8):
            rows = pl.ds(64 * x, 64)
            here = values[rows, :]
            edge = jnp.zeros((8, lanes), F32)
            beside = jnp.concatenate([edge, here[:-8]], axis=0) + jnp.concatenate(
                [here[8:], edge], axis=0
            )
            if x > 0:
                beside = beside + values[pl.ds(64 * (x - 1), 64), :]
            if x < 7:
                beside = beside + values[pl.ds(64 * (x + 1), 64), :]
            cube = here.reshape(8, 8, lanes)
            below = jnp.where(zrow == 0, 0.0, pltpu.roll(cube, 1, 1))
            above = jnp.where(zrow == 7, 0.0, pltpu.roll(cube, 7, 1))
            beside = beside + (below + above).reshape(64, lanes)
            applied_ref[rows, :] = 6.0 * here - beside

    def with_ghosts(ghost, use):
        zghost[pl.ds(0, 64, 8), :] = ghost(4, 0, 64)
        zghost[pl.ds(7, 64, 8), :] = ghost(5, 0, 64)
        for x in range(8):
            rows = pl.ds(64 * x, 64)
            outer = zghost[rows, :]
            if x == 0:
                outer = outer + ghost(0, 0, 64)
            if x == 7:
                outer = outer + ghost(1, 0, 64)
            outer = jnp.concatenate(
                [
                    outer[:8] + ghost(2, 8 * x, 8),
                    outer[8:56],
                    outer[56:] + ghost(3, 8 * x, 8),
                ],
                axis=0,
            )
            use(x, rows, outer)

    def stored(ghosts):
        return lambda face, start, size: ghosts[face, pl.ds(start, size), :]

    def prolonged(k):
        def ghost(face, start, size):
            return jnp.concatenate(
                [
                    doubled[k, face, pl.ds(8 * (a // 2), 8), :]
                    for a in range(start // 8, (start + size) // 8)
                ],
                axis=0,
            )

        return ghost

    def double(k, face, value):
        doubled[k, face, pl.ds(0, 16, 2), :] = value
        doubled[k, face, pl.ds(1, 16, 2), :] = value

    def coarse_outer(ghosts):
        zghost_coarse[pl.ds(0, 16, 4), :] = ghosts[4]
        zghost_coarse[pl.ds(3, 16, 4), :] = ghosts[5]
        for x in range(4):
            yghost_coarse[pl.ds(16 * x, 4), :] = ghosts[2, pl.ds(4 * x, 4), :]
            yghost_coarse[pl.ds(16 * x + 12, 4), :] = ghosts[3, pl.ds(4 * x, 4), :]
        outer = yghost_coarse[...] + zghost_coarse[...]
        return jnp.concatenate(
            [outer[:16] + ghosts[0], outer[16:48], outer[48:] + ghosts[1]], axis=0
        )

    exchange = fine_exchange(0)
    cut(first, 8, exchange.faces)
    pl.semaphore_wait(barrier, greeted)
    exchange.post()
    exchange.near()
    inner(first)
    exchange.forward()
    exchange.collect()

    def sweep(x, rows, outer):
        second[rows, :] = first[rows, :] + RELAX_FINE * (
            source[rows, :] - applied_ref[rows, :] + outer
        )

    with_ghosts(stored(exchange.ghosts), sweep)

    smoothed = fine_exchange(1)
    sampled = coarse_exchange(0)
    cut(second, 8, smoothed.faces)
    for direction in (0, 1):
        for k in range(12):
            halved[direction, pl.ds(8 * k, 8), :] = (
                smoothed.faces[direction, pl.ds(16 * k, 8), :]
                + smoothed.faces[direction, pl.ds(16 * k + 8, 8), :]
            )
        sampled.faces[direction, :, :] = (
            halved[direction, pl.ds(0, 48, 2), :] + halved[direction, pl.ds(1, 48, 2), :]
        )
    sampled.post()
    smoothed.post()
    sampled.near()
    inner(second)
    for x in range(0, 8, 2):
        lower, upper = pl.ds(64 * x, 64), pl.ds(64 * x + 64, 64)
        both = (source[lower, :] - applied_ref[lower, :]) + (
            source[upper, :] - applied_ref[upper, :]
        )
        for y in range(4):
            paired[pl.ds(32 * (x // 2) + 8 * y, 8), :] = (
                both[16 * y : 16 * y + 8] + both[16 * y + 8 : 16 * y + 16]
            )
    inner_rhs = paired[pl.ds(0, 64, 2), :] + paired[pl.ds(1, 64, 2), :]
    smoothed.near()
    sampled.forward()
    sampled.collect()
    coarse_rhs = 0.125 * (inner_rhs + coarse_outer(sampled.ghosts))
    coarse_one = RELAX_COARSE * coarse_rhs

    exchange = coarse_exchange(1)
    coarse = halved.at[0]
    coarse[0:64, :] = coarse_one
    cut(coarse, 4, exchange.faces)
    exchange.post()
    exchange.near()
    row = lax.broadcasted_iota(jnp.int32, (64, lanes), 0)
    edge = jnp.zeros((16, lanes), F32)
    beside = jnp.concatenate([edge, coarse_one[:-16]], axis=0) + jnp.concatenate(
        [coarse_one[16:], edge], axis=0
    )
    beside = beside + jnp.where(row // 4 % 4 == 0, 0.0, pltpu.roll(coarse_one, 4, 0))
    beside = beside + jnp.where(row // 4 % 4 == 3, 0.0, pltpu.roll(coarse_one, 60, 0))
    beside = beside + jnp.where(row % 4 == 0, 0.0, pltpu.roll(coarse_one, 1, 0))
    beside = beside + jnp.where(row % 4 == 3, 0.0, pltpu.roll(coarse_one, 63, 0))
    coarse_two = coarse_one + RELAX_COARSE * (coarse_rhs - 0.25 * (6.0 * coarse_one - beside))
    smoothed.forward()
    exchange.forward()
    exchange.collect()
    coarse_two = coarse_two + (0.25 * RELAX_COARSE) * coarse_outer(exchange.ghosts)

    corrected = coarse_exchange(2)
    coarse[0:64, :] = coarse_two
    cut(coarse, 4, corrected.faces)
    corrected.post()
    corrected.near()
    paired[pl.ds(0, 64, 2), :] = coarse_two
    paired[pl.ds(1, 64, 2), :] = coarse_two
    for x in range(8):
        for y in range(8):
            rows = pl.ds(64 * x + 8 * y, 8)
            lift = paired[pl.ds(32 * (x // 2) + 8 * (y // 2), 8), :]
            second[rows, :] = second[rows, :] + lift
    inner(second)
    smoothed.collect()

    def smooth(x, rows, outer):
        first[rows, :] = second[rows, :] + RELAX_FINE * (
            source[rows, :] - applied_ref[rows, :] + outer
        )

    with_ghosts(stored(smoothed.ghosts), smooth)
    almost = fine_exchange(2)
    cut(first, 8, almost.faces)
    almost.post()
    corrected.forward()
    corrected.collect()

    edges = coarse_exchange(3)
    for direction in (0, 1):
        at = 3 if direction == 0 else 0
        along_rows, across_rows = pl.ds(4 * at, 4), pl.ds(at, 4, 4)
        lines = [(g, along_rows) for g in (2, 3, 4, 5)]
        lines += [(g, along_rows) for g in (0, 1)] + [(g, across_rows) for g in (4, 5)]
        lines += [(g, across_rows) for g in (0, 1, 2, 3)]
        for k, (g, rows) in enumerate(lines):
            edges.faces[direction, pl.ds(4 * k, 4), :] = corrected.ghosts[g, rows, :]
    edges.post()
    edges.near()
    for face in range(6):
        double(0, face, corrected.ghosts[face])
        own = corrected.faces[1 - face % 2, pl.ds(16 * (face // 2), 16), :]
        double(1, face, jnp.where(hop_of[face : face + 1, :] >= 0, own, 0.0))

    def lift(x, rows, outer):
        first[rows, :] = first[rows, :] + RELAX_FINE * outer

    with_ghosts(prolonged(0), lift)
    inner(first)
    almost.near()
    almost.forward()
    almost.collect()
    outermost = almost.ghosts
    own = prolonged(1)
    for face in range(6):
        outermost[face] = outermost[face] + RELAX_FINE * own(face, 0, 64)
    edges.forward()
    edges.collect()
    for face in range(6):
        double(0, face, RELAX_FINE * edges.ghosts[face])
        for k, rows in enumerate((pl.ds(0, 8), pl.ds(56, 8), pl.ds(0, 8, 8), pl.ds(7, 8, 8))):
            outermost[face, rows, :] = (
                outermost[face, rows, :] + doubled[0, face, pl.ds(8 * k, 8), :]
            )

    parts = [jnp.zeros((8, lanes), F32)] * 5

    def fold(block):
        return jnp.sum(block.reshape(8, 8, lanes), axis=0)

    def close(x, rows, outer):
        here = first[rows, :]
        applied = applied_ref[rows, :] - outer
        image[rows, :] = applied
        r = source[rows, :]
        for k, term in enumerate((r * here, here * applied, r * r, r * applied, applied * applied)):
            parts[k] = parts[k] + fold(term)

    with_ghosts(stored(outermost), close)

    tile = jnp.zeros((1, lanes), F32)
    for k in range(5):
        one = jnp.sum(jnp.sum(parts[k], axis=0, keepdims=True), axis=1, keepdims=True)
        tile = jnp.where(lane == k, one, tile)
    base = 0
    for size, mine, peer in stages:
        sums[base + mine] = tile
        copies = []
        for k in range(1, size):
            made = pltpu.make_async_remote_copy(
                src_ref=sums.at[base + mine],
                dst_ref=sums.at[base + mine],
                send_sem=sum_send.at[base + k],
                recv_sem=sum_recv.at[base + k],
                device_id=peer(k),
                device_id_type=MESH,
            )
            made.start()
            copies.append(made)
        for made, sends in finishing:
            if sends is None:
                made.wait_send()
            else:
                pl.when(sends)(made.wait_send)
        finishing.clear()
        for made in copies:
            made.wait_recv()
        tile = jnp.sum(sums[base : base + size], axis=0)
        for made in copies:
            made.wait_send()
        base += size
    tile_ref[...] = tile


def finish(p_ref, image_ref, source_ref, tile_ref, sol_hbm, res_hbm, norm_ref, sol, res, sems):
    lanes = p_ref.shape[1]
    rows_per = p_ref.shape[0] // PIECES
    lane = lax.broadcasted_iota(jnp.int32, (1, lanes), 1)
    tile = tile_ref[...]
    along, curvature, old_square, cross, image_square = [
        jnp.sum(jnp.where(lane == k, tile, 0.0), axis=1, keepdims=True) for k in range(5)
    ]
    step = along / curvature
    copies = []
    for x in range(PIECES):
        rows = pl.ds(rows_per * x, rows_per)
        sol[rows, :] = step * p_ref[rows, :]
        res[rows, :] = source_ref[rows, :] - step * image_ref[rows, :]
        for k, (here, there) in enumerate(((sol, sol_hbm), (res, res_hbm))):
            made = pltpu.make_async_copy(here.at[rows], there.at[rows], sems.at[k, x])
            made.start()
            copies.append(made)
    square = old_square - 2.0 * step * cross + step * step * image_square
    norm_ref[0] = jnp.sqrt(square)[0, 0]
    for made in copies:
        made.wait()


def local(sizes, right_side, counts, neighbours):
    cells, lanes = right_side.shape
    curve_size, level_size = sizes
    total = curve_size * level_size

    def body(*refs):
        curve, level = lax.axis_index("curve"), lax.axis_index("level")
        if total <= 64:
            me = curve * level_size + level

            def everyone(k):
                other = (me + k) % total
                return (other // level_size, other % level_size)

            stages = [(total, me, everyone)]
        else:
            stages = [
                (level_size, level, lambda k: (curve, (level + k) % level_size)),
                (curve_size, curve, lambda k: ((curve + k) % curve_size, level)),
            ]
        kernel(sizes, stages, *refs)

    sum_rows = total if total <= 64 else curve_size + level_size
    vmem = pl.BlockSpec(memory_space=pltpu.VMEM)
    block = jax.ShapeDtypeStruct((cells, lanes), F32)
    whole = pltpu.VMEM((cells, lanes), F32)
    out = pl.pallas_call(
        body,
        out_shape=(whole, whole, whole, pltpu.VMEM((1, lanes), F32)),
        in_specs=[pl.BlockSpec(memory_space=pl.ANY)] * 3,
        out_specs=(vmem,) * 4,
        scratch_shapes=[
            pltpu.SMEM(counts.shape, jnp.int32),
            pltpu.VMEM(neighbours.shape, jnp.int32),
            pltpu.VMEM((cells, lanes), F32),
            pltpu.VMEM((cells, lanes), F32),
            pltpu.VMEM((cells // 4, lanes), F32),
            pltpu.VMEM((2, 96, lanes), F32),
            pltpu.VMEM((cells // 8, lanes), F32),
            pltpu.VMEM((cells // 8, lanes), F32),
            pltpu.VMEM((2, 6, 32, lanes), F32),
            pltpu.VMEM((cells, lanes), F32),
            pltpu.VMEM((3, 6, 64, lanes), F32),
            pltpu.VMEM((4, 6, 16, lanes), F32),
            pltpu.VMEM((3, 2, 192, lanes), F32),
            pltpu.VMEM((3, 96, lanes), F32),
            pltpu.VMEM((3, 2, HOPS, 192, lanes), F32),
            pltpu.VMEM((4, 2, 48, lanes), F32),
            pltpu.VMEM((4, 24, lanes), F32),
            pltpu.VMEM((4, 2, HOPS, 48, lanes), F32),
            pltpu.VMEM((sum_rows, 1, lanes), F32),
            pltpu.SemaphoreType.DMA((3,)),
            pltpu.SemaphoreType.DMA((7, 2, 3)),
            pltpu.SemaphoreType.DMA((7, 2, 3)),
            pltpu.SemaphoreType.DMA((7, 2, 3)),
            pltpu.SemaphoreType.DMA((7, 2, 3)),
            pltpu.SemaphoreType.DMA((7,)),
            pltpu.SemaphoreType.DMA((7,)),
            pltpu.SemaphoreType.DMA((7,)),
            pltpu.SemaphoreType.DMA((7,)),
            pltpu.SemaphoreType.DMA((sum_rows,)),
            pltpu.SemaphoreType.DMA((sum_rows,)),
        ],
        compiler_params=pltpu.CompilerParams(collective_id=0, has_side_effects=True),
    )(right_side, counts, neighbours)
    hbm = pl.BlockSpec(memory_space=pl.ANY)
    out = pl.pallas_call(
        finish,
        out_shape=(block, block, jax.ShapeDtypeStruct((1,), F32)),
        in_specs=[vmem] * 4,
        out_specs=(hbm, hbm, pl.BlockSpec(memory_space=pltpu.SMEM)),
        scratch_shapes=[
            pltpu.VMEM((cells, lanes), F32),
            pltpu.VMEM((cells, lanes), F32),
            pltpu.SemaphoreType.DMA((2, PIECES)),
        ],
    )(*[pltpu.with_memory_space_constraint(a, pltpu.VMEM) for a in out])
    return out[0], out[1], out[2].reshape(())


def solution(mesh):
    sizes = tuple(mesh.shape[name] for name in AXES)
    in_specs = (P(None, AXES), P(), P(None, AXES))
    out_specs = (P(None, AXES), P(None, AXES), P())
    return jax.shard_map(
        functools.partial(local, sizes), mesh=mesh, in_specs=in_specs, out_specs=out_specs, check_vma=False
    )
```

```python
import functools

import jax
import jax.numpy as jnp
from jax import lax
from jax.experimental import pallas as pl
from jax.experimental.pallas import tpu as pltpu
from jax.sharding import PartitionSpec as P

MIN_LIVE = 96
LAYER = 256
HOPS = 3
PIECES = 2
AXES = ("curve", "level")
MESH = pl.DeviceIdType.MESH
RELAXATION = 2.0 / 3.0
RELAX_FINE = RELAXATION / 6.0
RELAX_COARSE = RELAXATION / 1.5
F32 = jnp.float32


def kernel(
    sizes,
    stages,
    right_hbm,
    counts_hbm,
    neighbours_hbm,
    first,
    image,
    source,
    tile_ref,
    counts_ref,
    neighbours_ref,
    second,
    zghost,
    paired,
    halved,
    yghost_coarse,
    zghost_coarse,
    doubled,
    applied_ref,
    ghosts_fine,
    ghosts_coarse,
    faces_fine,
    packed_fine,
    windows_fine,
    faces_coarse,
    packed_coarse,
    windows_coarse,
    sums,
    loads,
    *sems,
):
    link_sems, relay_sems, pair_sems, far_sems, (sum_send, sum_recv) = [
        sems[i : i + 2] for i in range(0, 10, 2)
    ]
    curve_size, level_size = sizes
    total = curve_size * level_size
    me = lax.axis_index("curve") * level_size + lax.axis_index("level")
    lanes = source.shape[1]
    half = lanes // 2

    def place(index):
        return (index // level_size, index % level_size)

    inputs = [
        pltpu.make_async_copy(src, dst, loads.at[k])
        for k, (src, dst) in enumerate(
            ((right_hbm, second), (counts_hbm, counts_ref), (neighbours_hbm, neighbours_ref))
        )
    ]
    for made in inputs:
        made.start()
    barrier = pltpu.get_barrier_semaphore()
    greeted = 0
    if len(stages) > 1:
        for hop in range(1, HOPS + 1):
            for sign in (1, -1):
                target = (me + sign * hop + total) % total
                pl.semaphore_signal(barrier, inc=1, device_id=place(target), device_id_type=MESH)
                greeted += 1
    for size, _, peer in stages:
        for k in range(1, size):
            pl.semaphore_signal(barrier, inc=1, device_id=peer(k), device_id_type=MESH)
            greeted += 1
    zghost[...] = jnp.zeros_like(zghost)
    yghost_coarse[...] = jnp.zeros_like(yghost_coarse)
    zghost_coarse[...] = jnp.zeros_like(zghost_coarse)
    for made in inputs:
        made.wait()

    lane = lax.broadcasted_iota(jnp.int32, (1, lanes), 1)
    own_count = counts_ref[me]
    live = lane < own_count
    for x in range(8):
        rows = pl.ds(64 * x, 64)
        value = jnp.where(live, second[rows, :], 0.0)
        source[rows, :] = value
        first[rows, :] = RELAX_FINE * value

    nb = neighbours_ref[...]
    present = nb >= 0
    owner = nb // lanes
    offset = nb % lanes
    face_id = lax.broadcasted_iota(jnp.int32, nb.shape, 0)
    hop_of = jnp.where(face_id % 2 == 0, me - owner, owner - me)
    hop_of = jnp.where(present, hop_of, -1)
    far_count = counts_ref[jnp.maximum(me - HOPS, 0)]
    odd = me % 2
    even = 1 - odd
    partner = me + 1 - 2 * odd
    earlier_pair = me >= 2
    later_pair = me - odd + 2 < total
    reaches = (1 + 2 * even, 1 + 2 * odd)
    arrives = (2 * odd, 2 * even)
    far_there = jnp.where(odd == 1, me + HOPS < total, me >= HOPS)
    far_device = (me + HOPS * (2 * odd - 1) + total) % total
    skipped = jnp.where(
        (face_id % 2 == 0) & (hop_of == HOPS), even * (far_count - half), 0
    )
    where_at = jnp.clip(offset - skipped, 0, lanes - 1)
    low_half = jnp.broadcast_to(lane < half, (8, lanes))
    pack_index = jnp.broadcast_to(odd * (own_count - half) + lane % half, (8, lanes))

    def pick(block, index):
        return jnp.take_along_axis(block, index, axis=1, mode="promise_in_bounds")

    finishing = []

    def send(src, dst, sems, at, target, sends):
        made = pltpu.make_async_remote_copy(
            src_ref=src,
            dst_ref=dst,
            send_sem=sems[0].at[at],
            recv_sem=sems[1].at[at],
            device_id=place(target),
            device_id_type=MESH,
        )
        finishing.append((made, sends))
        return made

    def cut(values, extent, faces):
        area = extent * extent
        for direction in (0, 1):
            at = extent - 1 if direction == 0 else 0
            faces[direction, 0:area, :] = values[pl.ds(at * area, area), :]
            for x in range(extent):
                faces[direction, pl.ds(area + x * extent, extent), :] = values[
                    pl.ds(x * area + at * extent, extent), :
                ]
            faces[direction, pl.ds(2 * area, area), :] = values[pl.ds(at, area, extent), :]

    class Exchange:
        def __init__(self, stage, area, chunks, faces, packed, windows, ghosts):
            self.stage, self.area, self.chunks = stage, area, chunks
            self.faces, self.packed, self.windows, self.ghosts = faces, packed, windows, ghosts

        def post(self):
            faces, packed, windows, stage = self.faces, self.packed, self.windows, self.stage
            size = 3 * self.area // self.chunks
            pack = 3 * self.area // 2
            self.links = []
            for chunk in range(self.chunks):
                rows = pl.ds(chunk * size, size)
                for direction in (0, 1):
                    reach = reaches[direction]
                    target = me + reach if direction == 0 else me - reach
                    made = send(
                        faces.at[direction, rows],
                        windows.at[direction, reach - 1, rows],
                        link_sems,
                        (stage, direction, chunk),
                        (target + total) % total,
                        later_pair if direction == 0 else earlier_pair,
                    )
                    pl.when(later_pair if direction == 0 else earlier_pair)(made.start)
                    self.links.append((direction, chunk, rows, made))
            self.inside = send(
                faces.at[odd], windows.at[odd, 0], pair_sems, (stage,), partner, None
            )
            self.inside.start()
            for r in range(0, pack, 8):
                a = pick(faces[1 - odd, pl.ds(r, 8), :], pack_index)
                b = pick(faces[1 - odd, pl.ds(pack + r, 8), :], pack_index)
                packed[pl.ds(r, 8), :] = jnp.where(low_half, a, b)
            self.far = send(
                packed,
                windows.at[1 - odd, 2, pl.ds(0, pack)],
                far_sems,
                (stage,),
                far_device,
                far_there,
            )
            pl.when(far_there)(self.far.start)

        def pull(self, face, hops_in):
            area, faces, windows = self.area, self.faces, self.windows
            pack = 3 * area // 2
            direction, slot = face % 2, face // 2
            at = jnp.broadcast_to(where_at[face : face + 1, :], (8, lanes))
            is_packed = odd == direction
            at_high = jnp.where(is_packed, jnp.minimum(at + half, lanes - 1), at)
            hops = jnp.broadcast_to(hop_of[face : face + 1, :], (8, lanes))
            for r in range(0, area, 8):
                row = slot * area + r
                if 0 in hops_in:
                    block = jnp.zeros((8, lanes), F32)
                else:
                    block = self.ghosts[face, pl.ds(r, 8), :]
                for hop in hops_in:
                    index = at
                    if hop == 0:
                        window = faces[direction, pl.ds(row, 8), :]
                    elif hop < HOPS or row < pack:
                        window = windows[direction, hop - 1, pl.ds(row, 8), :]
                    else:
                        start = pl.multiple_of(row - jnp.where(is_packed, pack, 0), 8)
                        window = windows[direction, hop - 1, pl.ds(start, 8), :]
                        index = at_high
                    block = jnp.where(hops == hop, pick(window, index), block)
                self.ghosts[face, pl.ds(r, 8), :] = block

        def near(self):
            for face in range(6):
                self.pull(face, (0,))

        def forward(self):
            self.relays = {}
            for direction, chunk, rows, made in self.links:
                comes = earlier_pair if direction == 0 else later_pair
                relay = send(
                    self.windows.at[direction, arrives[direction], rows],
                    self.windows.at[direction, 1, rows],
                    relay_sems,
                    (self.stage, direction, chunk),
                    partner,
                    comes,
                )

                @pl.when(comes)
                def _():
                    made.wait_recv()
                    relay.start()

                self.relays[direction, chunk] = (relay, comes)

        def collect(self):
            self.inside.wait_recv()
            pl.when(far_there)(self.far.wait_recv)
            for face in range(6):
                waits = self.relays.pop((face % 2, face // 2), None)
                if waits is not None:
                    relay, comes = waits
                    pl.when(comes)(relay.wait_recv)
                self.pull(face, (1, 2, 3))

    def fine_exchange(k):
        return Exchange(
            k, 64, 3, faces_fine.at[k], packed_fine.at[k], windows_fine.at[k], ghosts_fine.at[k]
        )

    def coarse_exchange(k):
        return Exchange(
            3 + k,
            16,
            1,
            faces_coarse.at[k],
            packed_coarse.at[k],
            windows_coarse.at[k],
            ghosts_coarse.at[k],
        )

    zrow = lax.broadcasted_iota(jnp.int32, (8, 8, lanes), 1)

    def inner(values):
        for x in range(8):
            rows = pl.ds(64 * x, 64)
            here = values[rows, :]
            edge = jnp.zeros((8, lanes), F32)
            beside = jnp.concatenate([edge, here[:-8]], axis=0) + jnp.concatenate(
                [here[8:], edge], axis=0
            )
            if x > 0:
                beside = beside + values[pl.ds(64 * (x - 1), 64), :]
            if x < 7:
                beside = beside + values[pl.ds(64 * (x + 1), 64), :]
            cube = here.reshape(8, 8, lanes)
            below = jnp.where(zrow == 0, 0.0, pltpu.roll(cube, 1, 1))
            above = jnp.where(zrow == 7, 0.0, pltpu.roll(cube, 7, 1))
            beside = beside + (below + above).reshape(64, lanes)
            applied_ref[rows, :] = 6.0 * here - beside

    def with_ghosts(ghost, use):
        zghost[pl.ds(0, 64, 8), :] = ghost(4, 0, 64)
        zghost[pl.ds(7, 64, 8), :] = ghost(5, 0, 64)
        for x in range(8):
            rows = pl.ds(64 * x, 64)
            outer = zghost[rows, :]
            if x == 0:
                outer = outer + ghost(0, 0, 64)
            if x == 7:
                outer = outer + ghost(1, 0, 64)
            outer = jnp.concatenate(
                [
                    outer[:8] + ghost(2, 8 * x, 8),
                    outer[8:56],
                    outer[56:] + ghost(3, 8 * x, 8),
                ],
                axis=0,
            )
            use(x, rows, outer)

    def stored(ghosts):
        return lambda face, start, size: ghosts[face, pl.ds(start, size), :]

    def prolonged(k):
        def ghost(face, start, size):
            return jnp.concatenate(
                [
                    doubled[k, face, pl.ds(8 * (a // 2), 8), :]
                    for a in range(start // 8, (start + size) // 8)
                ],
                axis=0,
            )

        return ghost

    def double(k, face, value):
        doubled[k, face, pl.ds(0, 16, 2), :] = value
        doubled[k, face, pl.ds(1, 16, 2), :] = value

    def coarse_outer(ghosts):
        zghost_coarse[pl.ds(0, 16, 4), :] = ghosts[4]
        zghost_coarse[pl.ds(3, 16, 4), :] = ghosts[5]
        for x in range(4):
            yghost_coarse[pl.ds(16 * x, 4), :] = ghosts[2, pl.ds(4 * x, 4), :]
            yghost_coarse[pl.ds(16 * x + 12, 4), :] = ghosts[3, pl.ds(4 * x, 4), :]
        outer = yghost_coarse[...] + zghost_coarse[...]
        return jnp.concatenate(
            [outer[:16] + ghosts[0], outer[16:48], outer[48:] + ghosts[1]], axis=0
        )

    exchange = fine_exchange(0)
    cut(first, 8, exchange.faces)
    pl.semaphore_wait(barrier, greeted)
    exchange.post()
    exchange.near()
    inner(first)
    exchange.forward()
    exchange.collect()

    def sweep(x, rows, outer):
        second[rows, :] = first[rows, :] + RELAX_FINE * (
            source[rows, :] - applied_ref[rows, :] + outer
        )

    with_ghosts(stored(exchange.ghosts), sweep)

    smoothed = fine_exchange(1)
    sampled = coarse_exchange(0)
    cut(second, 8, smoothed.faces)
    for direction in (0, 1):
        for k in range(12):
            halved[direction, pl.ds(8 * k, 8), :] = (
                smoothed.faces[direction, pl.ds(16 * k, 8), :]
                + smoothed.faces[direction, pl.ds(16 * k + 8, 8), :]
            )
        sampled.faces[direction, :, :] = (
            halved[direction, pl.ds(0, 48, 2), :] + halved[direction, pl.ds(1, 48, 2), :]
        )
    sampled.post()
    smoothed.post()
    sampled.near()
    inner(second)
    for x in range(0, 8, 2):
        lower, upper = pl.ds(64 * x, 64), pl.ds(64 * x + 64, 64)
        both = (source[lower, :] - applied_ref[lower, :]) + (
            source[upper, :] - applied_ref[upper, :]
        )
        for y in range(4):
            paired[pl.ds(32 * (x // 2) + 8 * y, 8), :] = (
                both[16 * y : 16 * y + 8] + both[16 * y + 8 : 16 * y + 16]
            )
    inner_rhs = paired[pl.ds(0, 64, 2), :] + paired[pl.ds(1, 64, 2), :]
    smoothed.near()
    sampled.forward()
    sampled.collect()
    coarse_rhs = 0.125 * (inner_rhs + coarse_outer(sampled.ghosts))
    coarse_one = RELAX_COARSE * coarse_rhs

    exchange = coarse_exchange(1)
    coarse = halved.at[0]
    coarse[0:64, :] = coarse_one
    cut(coarse, 4, exchange.faces)
    exchange.post()
    exchange.near()
    row = lax.broadcasted_iota(jnp.int32, (64, lanes), 0)
    edge = jnp.zeros((16, lanes), F32)
    beside = jnp.concatenate([edge, coarse_one[:-16]], axis=0) + jnp.concatenate(
        [coarse_one[16:], edge], axis=0
    )
    beside = beside + jnp.where(row // 4 % 4 == 0, 0.0, pltpu.roll(coarse_one, 4, 0))
    beside = beside + jnp.where(row // 4 % 4 == 3, 0.0, pltpu.roll(coarse_one, 60, 0))
    beside = beside + jnp.where(row % 4 == 0, 0.0, pltpu.roll(coarse_one, 1, 0))
    beside = beside + jnp.where(row % 4 == 3, 0.0, pltpu.roll(coarse_one, 63, 0))
    coarse_two = coarse_one + RELAX_COARSE * (coarse_rhs - 0.25 * (6.0 * coarse_one - beside))
    smoothed.forward()
    exchange.forward()
    exchange.collect()
    coarse_two = coarse_two + (0.25 * RELAX_COARSE) * coarse_outer(exchange.ghosts)

    corrected = coarse_exchange(2)
    coarse[0:64, :] = coarse_two
    cut(coarse, 4, corrected.faces)
    corrected.post()
    corrected.near()
    paired[pl.ds(0, 64, 2), :] = coarse_two
    paired[pl.ds(1, 64, 2), :] = coarse_two
    for x in range(8):
        for y in range(8):
            rows = pl.ds(64 * x + 8 * y, 8)
            lift = paired[pl.ds(32 * (x // 2) + 8 * (y // 2), 8), :]
            second[rows, :] = second[rows, :] + lift
    inner(second)
    smoothed.collect()

    def smooth(x, rows, outer):
        first[rows, :] = second[rows, :] + RELAX_FINE * (
            source[rows, :] - applied_ref[rows, :] + outer
        )

    with_ghosts(stored(smoothed.ghosts), smooth)
    almost = fine_exchange(2)
    cut(first, 8, almost.faces)
    almost.post()
    corrected.forward()
    corrected.collect()

    edges = coarse_exchange(3)
    for direction in (0, 1):
        at = 3 if direction == 0 else 0
        along_rows, across_rows = pl.ds(4 * at, 4), pl.ds(at, 4, 4)
        lines = [(g, along_rows) for g in (2, 3, 4, 5)]
        lines += [(g, along_rows) for g in (0, 1)] + [(g, across_rows) for g in (4, 5)]
        lines += [(g, across_rows) for g in (0, 1, 2, 3)]
        for k, (g, rows) in enumerate(lines):
            edges.faces[direction, pl.ds(4 * k, 4), :] = corrected.ghosts[g, rows, :]
    edges.post()
    edges.near()
    for face in range(6):
        double(0, face, corrected.ghosts[face])
        own = corrected.faces[1 - face % 2, pl.ds(16 * (face // 2), 16), :]
        double(1, face, jnp.where(hop_of[face : face + 1, :] >= 0, own, 0.0))

    def lift(x, rows, outer):
        first[rows, :] = first[rows, :] + RELAX_FINE * outer

    with_ghosts(prolonged(0), lift)
    inner(first)
    almost.near()
    almost.forward()
    almost.collect()
    outermost = almost.ghosts
    own = prolonged(1)
    for face in range(6):
        outermost[face] = outermost[face] + RELAX_FINE * own(face, 0, 64)
    edges.forward()
    edges.collect()
    for face in range(6):
        double(0, face, RELAX_FINE * edges.ghosts[face])
        for k, rows in enumerate((pl.ds(0, 8), pl.ds(56, 8), pl.ds(0, 8, 8), pl.ds(7, 8, 8))):
            outermost[face, rows, :] = (
                outermost[face, rows, :] + doubled[0, face, pl.ds(8 * k, 8), :]
            )

    parts = [jnp.zeros((8, lanes), F32)] * 5

    def fold(block):
        return jnp.sum(block.reshape(8, 8, lanes), axis=0)

    def close(x, rows, outer):
        here = first[rows, :]
        applied = applied_ref[rows, :] - outer
        image[rows, :] = applied
        r = source[rows, :]
        for k, term in enumerate((r * here, here * applied, r * r, r * applied, applied * applied)):
            parts[k] = parts[k] + fold(term)

    with_ghosts(stored(outermost), close)

    tile = jnp.zeros((1, lanes), F32)
    for k in range(5):
        one = jnp.sum(jnp.sum(parts[k], axis=0, keepdims=True), axis=1, keepdims=True)
        tile = jnp.where(lane == k, one, tile)
    base = 0
    for stage, (size, mine, peer) in enumerate(stages):
        sums[base + mine] = tile
        for k in range(1, size):
            made = pltpu.make_async_remote_copy(
                src_ref=sums.at[base + mine],
                dst_ref=sums.at[base + mine],
                send_sem=sum_send.at[stage],
                recv_sem=sum_recv.at[stage],
                device_id=peer(k),
                device_id_type=MESH,
            )
            made.start()
        arriving = sums.at[pl.ds(base, size - 1)]
        for made, sends in finishing:
            if sends is None:
                made.wait_send()
            else:
                pl.when(sends)(made.wait_send)
        finishing.clear()
        pltpu.make_async_copy(arriving, arriving, sum_send.at[stage]).wait()
        pltpu.make_async_copy(arriving, arriving, sum_recv.at[stage]).wait()
        tile = jnp.sum(sums[base : base + size], axis=0)
        base += size
    tile_ref[...] = tile


def finish(p_ref, image_ref, source_ref, tile_ref, sol_hbm, res_hbm, norm_ref, sol, res, sems):
    lanes = p_ref.shape[1]
    rows_per = p_ref.shape[0] // PIECES
    lane = lax.broadcasted_iota(jnp.int32, (1, lanes), 1)
    tile = tile_ref[...]
    along, curvature, old_square, cross, image_square = [
        jnp.sum(jnp.where(lane == k, tile, 0.0), axis=1, keepdims=True) for k in range(5)
    ]
    step = along / curvature
    copies = []
    for x in range(PIECES):
        rows = pl.ds(rows_per * x, rows_per)
        sol[rows, :] = step * p_ref[rows, :]
        res[rows, :] = source_ref[rows, :] - step * image_ref[rows, :]
        for k, (here, there) in enumerate(((sol, sol_hbm), (res, res_hbm))):
            made = pltpu.make_async_copy(here.at[rows], there.at[rows], sems.at[k, x])
            made.start()
            copies.append(made)
    square = old_square - 2.0 * step * cross + step * step * image_square
    norm_ref[0] = jnp.sqrt(square)[0, 0]
    for made in copies:
        made.wait()


def local(sizes, right_side, counts, neighbours):
    cells, lanes = right_side.shape
    curve_size, level_size = sizes
    total = curve_size * level_size

    def body(*refs):
        curve, level = lax.axis_index("curve"), lax.axis_index("level")
        if total <= 64:
            me = curve * level_size + level

            def everyone(k):
                other = (me + k) % total
                return (other // level_size, other % level_size)

            stages = [(total, me, everyone)]
        else:
            stages = [
                (level_size, level, lambda k: (curve, (level + k) % level_size)),
                (curve_size, curve, lambda k: ((curve + k) % curve_size, level)),
            ]
        kernel(sizes, stages, *refs)

    sum_rows = total if total <= 64 else curve_size + level_size
    vmem = pl.BlockSpec(memory_space=pltpu.VMEM)
    block = jax.ShapeDtypeStruct((cells, lanes), F32)
    whole = pltpu.VMEM((cells, lanes), F32)
    out = pl.pallas_call(
        body,
        out_shape=(whole, whole, whole, pltpu.VMEM((1, lanes), F32)),
        in_specs=[pl.BlockSpec(memory_space=pl.ANY)] * 3,
        out_specs=(vmem,) * 4,
        scratch_shapes=[
            pltpu.SMEM(counts.shape, jnp.int32),
            pltpu.VMEM(neighbours.shape, jnp.int32),
            pltpu.VMEM((cells, lanes), F32),
            pltpu.VMEM((cells, lanes), F32),
            pltpu.VMEM((cells // 4, lanes), F32),
            pltpu.VMEM((2, 96, lanes), F32),
            pltpu.VMEM((cells // 8, lanes), F32),
            pltpu.VMEM((cells // 8, lanes), F32),
            pltpu.VMEM((2, 6, 32, lanes), F32),
            pltpu.VMEM((cells, lanes), F32),
            pltpu.VMEM((3, 6, 64, lanes), F32),
            pltpu.VMEM((4, 6, 16, lanes), F32),
            pltpu.VMEM((3, 2, 192, lanes), F32),
            pltpu.VMEM((3, 96, lanes), F32),
            pltpu.VMEM((3, 2, HOPS, 192, lanes), F32),
            pltpu.VMEM((4, 2, 48, lanes), F32),
            pltpu.VMEM((4, 24, lanes), F32),
            pltpu.VMEM((4, 2, HOPS, 48, lanes), F32),
            pltpu.VMEM((sum_rows, 1, lanes), F32),
            pltpu.SemaphoreType.DMA((3,)),
            pltpu.SemaphoreType.DMA((7, 2, 3)),
            pltpu.SemaphoreType.DMA((7, 2, 3)),
            pltpu.SemaphoreType.DMA((7, 2, 3)),
            pltpu.SemaphoreType.DMA((7, 2, 3)),
            pltpu.SemaphoreType.DMA((7,)),
            pltpu.SemaphoreType.DMA((7,)),
            pltpu.SemaphoreType.DMA((7,)),
            pltpu.SemaphoreType.DMA((7,)),
            pltpu.SemaphoreType.DMA((2,)),
            pltpu.SemaphoreType.DMA((2,)),
        ],
        compiler_params=pltpu.CompilerParams(collective_id=0, has_side_effects=True),
    )(right_side, counts, neighbours)
    hbm = pl.BlockSpec(memory_space=pl.ANY)
    out = pl.pallas_call(
        finish,
        out_shape=(block, block, jax.ShapeDtypeStruct((1,), F32)),
        in_specs=[vmem] * 4,
        out_specs=(hbm, hbm, pl.BlockSpec(memory_space=pltpu.SMEM)),
        scratch_shapes=[
            pltpu.VMEM((cells, lanes), F32),
            pltpu.VMEM((cells, lanes), F32),
            pltpu.SemaphoreType.DMA((2, PIECES)),
        ],
    )(*[pltpu.with_memory_space_constraint(a, pltpu.VMEM) for a in out])
    return out[0], out[1], out[2].reshape(())


def solution(mesh):
    sizes = tuple(mesh.shape[name] for name in AXES)
    in_specs = (P(None, AXES), P(), P(None, AXES))
    out_specs = (P(None, AXES), P(None, AXES), P())
    return jax.shard_map(
        functools.partial(local, sizes), mesh=mesh, in_specs=in_specs, out_specs=out_specs, check_vma=False
    )
```

```python
import functools

import jax
import jax.numpy as jnp
from jax import lax
from jax.experimental import pallas as pl
from jax.experimental.pallas import tpu as pltpu
from jax.sharding import PartitionSpec as P

MIN_LIVE = 96
LAYER = 256
HOPS = 3
PIECES = 2
AXES = ("curve", "level")
MESH = pl.DeviceIdType.MESH
RELAXATION = 2.0 / 3.0
RELAX_FINE = RELAXATION / 6.0
RELAX_COARSE = RELAXATION / 1.5
F32 = jnp.float32


def kernel(
    sizes,
    stages,
    group_size,
    right_hbm,
    counts_hbm,
    neighbours_hbm,
    first,
    image,
    source,
    tile_ref,
    counts_ref,
    neighbours_ref,
    second,
    zghost,
    paired,
    halved,
    yghost_coarse,
    zghost_coarse,
    doubled,
    applied_ref,
    ghosts_fine,
    ghosts_coarse,
    faces_fine,
    packed_fine,
    windows_fine,
    faces_coarse,
    packed_coarse,
    windows_coarse,
    sums,
    loads,
    words,
    *sems,
):
    link_sems, relay_sems, pair_sems, far_sems, (sum_send, sum_recv) = [
        sems[i : i + 2] for i in range(0, 10, 2)
    ]
    curve_size, level_size = sizes
    total = curve_size * level_size
    me = lax.axis_index("curve") * level_size + lax.axis_index("level")
    lanes = source.shape[1]
    half = lanes // 2

    def place(index):
        return (index // level_size, index % level_size)

    inputs = [
        pltpu.make_async_copy(src, dst, loads.at[k])
        for k, (src, dst) in enumerate(
            ((right_hbm, second), (counts_hbm, counts_ref), (neighbours_hbm, neighbours_ref))
        )
    ]
    for made in inputs:
        made.start()
    barrier = pltpu.get_barrier_semaphore()
    greeted = 0
    groups = total // group_size
    group = me // group_size
    if len(stages) > 1:
        for hop in range(1, HOPS + 1):
            for sign in (1, -1):
                target = (me + sign * hop + total) % total
                pl.semaphore_signal(barrier, inc=1, device_id=place(target), device_id_type=MESH)
                greeted += 1
        for size, _, peer in stages:
            for k in range(1, size):
                pl.semaphore_signal(barrier, inc=1, device_id=peer(k), device_id_type=MESH)
                greeted += 1
    else:
        for hop in sorted({*range(1, HOPS + 1), *range(1, group_size + 1)}):
            for sign in (1, -1):
                target = me + sign * hop
                there = (target >= 0) & (target < total)
                if HOPS < hop < group_size:
                    there = there & ((target + total) // group_size == group + groups)

                @pl.when(there)
                def _():
                    pl.semaphore_signal(
                        barrier,
                        inc=1,
                        device_id=place((target + total) % total),
                        device_id_type=MESH,
                    )

                greeted = greeted + there.astype(jnp.int32)

    def pass_word(step):
        if len(stages) > 1 or step > groups:
            return
        sides = ((0, 1, group), (1, -1, groups - 1 - group))
        if step > 1:
            for side, _, known in sides:

                @pl.when(known >= step - 1)
                def _():
                    pl.semaphore_wait(words.at[side, step - 2], 1)

        if step < groups:
            for side, sign, known in sides:
                target = me + sign * group_size

                @pl.when((known >= step - 1) & (target >= 0) & (target < total))
                def _():
                    pl.semaphore_signal(
                        words.at[side, step - 1],
                        inc=1,
                        device_id=place((target + total) % total),
                        device_id_type=MESH,
                    )

    zghost[...] = jnp.zeros_like(zghost)
    yghost_coarse[...] = jnp.zeros_like(yghost_coarse)
    zghost_coarse[...] = jnp.zeros_like(zghost_coarse)
    for made in inputs:
        made.wait()

    lane = lax.broadcasted_iota(jnp.int32, (1, lanes), 1)
    own_count = counts_ref[me]
    live = lane < own_count
    for x in range(8):
        rows = pl.ds(64 * x, 64)
        value = jnp.where(live, second[rows, :], 0.0)
        source[rows, :] = value
        first[rows, :] = RELAX_FINE * value

    nb = neighbours_ref[...]
    present = nb >= 0
    owner = nb // lanes
    offset = nb % lanes
    face_id = lax.broadcasted_iota(jnp.int32, nb.shape, 0)
    hop_of = jnp.where(face_id % 2 == 0, me - owner, owner - me)
    hop_of = jnp.where(present, hop_of, -1)
    far_count = counts_ref[jnp.maximum(me - HOPS, 0)]
    odd = me % 2
    even = 1 - odd
    partner = me + 1 - 2 * odd
    earlier_pair = me >= 2
    later_pair = me - odd + 2 < total
    reaches = (1 + 2 * even, 1 + 2 * odd)
    arrives = (2 * odd, 2 * even)
    far_there = jnp.where(odd == 1, me + HOPS < total, me >= HOPS)
    far_device = (me + HOPS * (2 * odd - 1) + total) % total
    skipped = jnp.where(
        (face_id % 2 == 0) & (hop_of == HOPS), even * (far_count - half), 0
    )
    where_at = jnp.clip(offset - skipped, 0, lanes - 1)
    low_half = jnp.broadcast_to(lane < half, (8, lanes))
    pack_index = jnp.broadcast_to(odd * (own_count - half) + lane % half, (8, lanes))

    def pick(block, index):
        return jnp.take_along_axis(block, index, axis=1, mode="promise_in_bounds")

    finishing = []

    def send(src, dst, sems, at, target, sends):
        made = pltpu.make_async_remote_copy(
            src_ref=src,
            dst_ref=dst,
            send_sem=sems[0].at[at],
            recv_sem=sems[1].at[at],
            device_id=place(target),
            device_id_type=MESH,
        )
        finishing.append((made, sends))
        return made

    def cut(values, extent, faces):
        area = extent * extent
        for direction in (0, 1):
            at = extent - 1 if direction == 0 else 0
            faces[direction, 0:area, :] = values[pl.ds(at * area, area), :]
            for x in range(extent):
                faces[direction, pl.ds(area + x * extent, extent), :] = values[
                    pl.ds(x * area + at * extent, extent), :
                ]
            faces[direction, pl.ds(2 * area, area), :] = values[pl.ds(at, area, extent), :]

    class Exchange:
        def __init__(self, stage, area, chunks, faces, packed, windows, ghosts):
            self.stage, self.area, self.chunks = stage, area, chunks
            self.faces, self.packed, self.windows, self.ghosts = faces, packed, windows, ghosts

        def post(self):
            faces, packed, windows, stage = self.faces, self.packed, self.windows, self.stage
            size = 3 * self.area // self.chunks
            pack = 3 * self.area // 2
            self.links = []
            for chunk in range(self.chunks):
                rows = pl.ds(chunk * size, size)
                for direction in (0, 1):
                    reach = reaches[direction]
                    target = me + reach if direction == 0 else me - reach
                    made = send(
                        faces.at[direction, rows],
                        windows.at[direction, reach - 1, rows],
                        link_sems,
                        (stage, direction, chunk),
                        (target + total) % total,
                        later_pair if direction == 0 else earlier_pair,
                    )
                    pl.when(later_pair if direction == 0 else earlier_pair)(made.start)
                    self.links.append((direction, chunk, rows, made))
            self.inside = send(
                faces.at[odd], windows.at[odd, 0], pair_sems, (stage,), partner, None
            )
            self.inside.start()
            for r in range(0, pack, 8):
                a = pick(faces[1 - odd, pl.ds(r, 8), :], pack_index)
                b = pick(faces[1 - odd, pl.ds(pack + r, 8), :], pack_index)
                packed[pl.ds(r, 8), :] = jnp.where(low_half, a, b)
            self.far = send(
                packed,
                windows.at[1 - odd, 2, pl.ds(0, pack)],
                far_sems,
                (stage,),
                far_device,
                far_there,
            )
            pl.when(far_there)(self.far.start)

        def pull(self, face, hops_in):
            area, faces, windows = self.area, self.faces, self.windows
            pack = 3 * area // 2
            direction, slot = face % 2, face // 2
            at = jnp.broadcast_to(where_at[face : face + 1, :], (8, lanes))
            is_packed = odd == direction
            at_high = jnp.where(is_packed, jnp.minimum(at + half, lanes - 1), at)
            hops = jnp.broadcast_to(hop_of[face : face + 1, :], (8, lanes))
            for r in range(0, area, 8):
                row = slot * area + r
                if 0 in hops_in:
                    block = jnp.zeros((8, lanes), F32)
                else:
                    block = self.ghosts[face, pl.ds(r, 8), :]
                for hop in hops_in:
                    index = at
                    if hop == 0:
                        window = faces[direction, pl.ds(row, 8), :]
                    elif hop < HOPS or row < pack:
                        window = windows[direction, hop - 1, pl.ds(row, 8), :]
                    else:
                        start = pl.multiple_of(row - jnp.where(is_packed, pack, 0), 8)
                        window = windows[direction, hop - 1, pl.ds(start, 8), :]
                        index = at_high
                    block = jnp.where(hops == hop, pick(window, index), block)
                self.ghosts[face, pl.ds(r, 8), :] = block

        def near(self):
            for face in range(6):
                self.pull(face, (0,))

        def forward(self):
            self.relays = {}
            for direction, chunk, rows, made in self.links:
                comes = earlier_pair if direction == 0 else later_pair
                relay = send(
                    self.windows.at[direction, arrives[direction], rows],
                    self.windows.at[direction, 1, rows],
                    relay_sems,
                    (self.stage, direction, chunk),
                    partner,
                    comes,
                )

                @pl.when(comes)
                def _():
                    made.wait_recv()
                    relay.start()

                self.relays[direction, chunk] = (relay, comes)

        def collect(self):
            self.inside.wait_recv()
            pl.when(far_there)(self.far.wait_recv)
            for face in range(6):
                waits = self.relays.pop((face % 2, face // 2), None)
                if waits is not None:
                    relay, comes = waits
                    pl.when(comes)(relay.wait_recv)
                self.pull(face, (1, 2, 3))

    def fine_exchange(k):
        return Exchange(
            k, 64, 3, faces_fine.at[k], packed_fine.at[k], windows_fine.at[k], ghosts_fine.at[k]
        )

    def coarse_exchange(k):
        return Exchange(
            3 + k,
            16,
            1,
            faces_coarse.at[k],
            packed_coarse.at[k],
            windows_coarse.at[k],
            ghosts_coarse.at[k],
        )

    zrow = lax.broadcasted_iota(jnp.int32, (8, 8, lanes), 1)

    def inner(values):
        for x in range(8):
            rows = pl.ds(64 * x, 64)
            here = values[rows, :]
            edge = jnp.zeros((8, lanes), F32)
            beside = jnp.concatenate([edge, here[:-8]], axis=0) + jnp.concatenate(
                [here[8:], edge], axis=0
            )
            if x > 0:
                beside = beside + values[pl.ds(64 * (x - 1), 64), :]
            if x < 7:
                beside = beside + values[pl.ds(64 * (x + 1), 64), :]
            cube = here.reshape(8, 8, lanes)
            below = jnp.where(zrow == 0, 0.0, pltpu.roll(cube, 1, 1))
            above = jnp.where(zrow == 7, 0.0, pltpu.roll(cube, 7, 1))
            beside = beside + (below + above).reshape(64, lanes)
            applied_ref[rows, :] = 6.0 * here - beside

    def with_ghosts(ghost, use):
        zghost[pl.ds(0, 64, 8), :] = ghost(4, 0, 64)
        zghost[pl.ds(7, 64, 8), :] = ghost(5, 0, 64)
        for x in range(8):
            rows = pl.ds(64 * x, 64)
            outer = zghost[rows, :]
            if x == 0:
                outer = outer + ghost(0, 0, 64)
            if x == 7:
                outer = outer + ghost(1, 0, 64)
            outer = jnp.concatenate(
                [
                    outer[:8] + ghost(2, 8 * x, 8),
                    outer[8:56],
                    outer[56:] + ghost(3, 8 * x, 8),
                ],
                axis=0,
            )
            use(x, rows, outer)

    def stored(ghosts):
        return lambda face, start, size: ghosts[face, pl.ds(start, size), :]

    def prolonged(k):
        def ghost(face, start, size):
            return jnp.concatenate(
                [
                    doubled[k, face, pl.ds(8 * (a // 2), 8), :]
                    for a in range(start // 8, (start + size) // 8)
                ],
                axis=0,
            )

        return ghost

    def double(k, face, value):
        doubled[k, face, pl.ds(0, 16, 2), :] = value
        doubled[k, face, pl.ds(1, 16, 2), :] = value

    def coarse_outer(ghosts):
        zghost_coarse[pl.ds(0, 16, 4), :] = ghosts[4]
        zghost_coarse[pl.ds(3, 16, 4), :] = ghosts[5]
        for x in range(4):
            yghost_coarse[pl.ds(16 * x, 4), :] = ghosts[2, pl.ds(4 * x, 4), :]
            yghost_coarse[pl.ds(16 * x + 12, 4), :] = ghosts[3, pl.ds(4 * x, 4), :]
        outer = yghost_coarse[...] + zghost_coarse[...]
        return jnp.concatenate(
            [outer[:16] + ghosts[0], outer[16:48], outer[48:] + ghosts[1]], axis=0
        )

    exchange = fine_exchange(0)
    cut(first, 8, exchange.faces)
    pl.semaphore_wait(barrier, greeted)
    exchange.post()
    pass_word(1)
    exchange.near()
    inner(first)
    exchange.forward()
    pass_word(2)
    exchange.collect()

    def sweep(x, rows, outer):
        second[rows, :] = first[rows, :] + RELAX_FINE * (
            source[rows, :] - applied_ref[rows, :] + outer
        )

    with_ghosts(stored(exchange.ghosts), sweep)

    smoothed = fine_exchange(1)
    sampled = coarse_exchange(0)
    cut(second, 8, smoothed.faces)
    for direction in (0, 1):
        for k in range(12):
            halved[direction, pl.ds(8 * k, 8), :] = (
                smoothed.faces[direction, pl.ds(16 * k, 8), :]
                + smoothed.faces[direction, pl.ds(16 * k + 8, 8), :]
            )
        sampled.faces[direction, :, :] = (
            halved[direction, pl.ds(0, 48, 2), :] + halved[direction, pl.ds(1, 48, 2), :]
        )
    sampled.post()
    smoothed.post()
    sampled.near()
    inner(second)
    for x in range(0, 8, 2):
        lower, upper = pl.ds(64 * x, 64), pl.ds(64 * x + 64, 64)
        both = (source[lower, :] - applied_ref[lower, :]) + (
            source[upper, :] - applied_ref[upper, :]
        )
        for y in range(4):
            paired[pl.ds(32 * (x // 2) + 8 * y, 8), :] = (
                both[16 * y : 16 * y + 8] + both[16 * y + 8 : 16 * y + 16]
            )
    inner_rhs = paired[pl.ds(0, 64, 2), :] + paired[pl.ds(1, 64, 2), :]
    smoothed.near()
    sampled.forward()
    pass_word(3)
    sampled.collect()
    coarse_rhs = 0.125 * (inner_rhs + coarse_outer(sampled.ghosts))
    coarse_one = RELAX_COARSE * coarse_rhs

    exchange = coarse_exchange(1)
    coarse = halved.at[0]
    coarse[0:64, :] = coarse_one
    cut(coarse, 4, exchange.faces)
    exchange.post()
    exchange.near()
    row = lax.broadcasted_iota(jnp.int32, (64, lanes), 0)
    edge = jnp.zeros((16, lanes), F32)
    beside = jnp.concatenate([edge, coarse_one[:-16]], axis=0) + jnp.concatenate(
        [coarse_one[16:], edge], axis=0
    )
    beside = beside + jnp.where(row // 4 % 4 == 0, 0.0, pltpu.roll(coarse_one, 4, 0))
    beside = beside + jnp.where(row // 4 % 4 == 3, 0.0, pltpu.roll(coarse_one, 60, 0))
    beside = beside + jnp.where(row % 4 == 0, 0.0, pltpu.roll(coarse_one, 1, 0))
    beside = beside + jnp.where(row % 4 == 3, 0.0, pltpu.roll(coarse_one, 63, 0))
    coarse_two = coarse_one + RELAX_COARSE * (coarse_rhs - 0.25 * (6.0 * coarse_one - beside))
    smoothed.forward()
    exchange.forward()
    for step in range(4, total // group_size + 1):
        pass_word(step)
    exchange.collect()
    coarse_two = coarse_two + (0.25 * RELAX_COARSE) * coarse_outer(exchange.ghosts)

    corrected = coarse_exchange(2)
    coarse[0:64, :] = coarse_two
    cut(coarse, 4, corrected.faces)
    corrected.post()
    corrected.near()
    paired[pl.ds(0, 64, 2), :] = coarse_two
    paired[pl.ds(1, 64, 2), :] = coarse_two
    for x in range(8):
        for y in range(8):
            rows = pl.ds(64 * x + 8 * y, 8)
            lift = paired[pl.ds(32 * (x // 2) + 8 * (y // 2), 8), :]
            second[rows, :] = second[rows, :] + lift
    inner(second)
    smoothed.collect()

    def smooth(x, rows, outer):
        first[rows, :] = second[rows, :] + RELAX_FINE * (
            source[rows, :] - applied_ref[rows, :] + outer
        )

    with_ghosts(stored(smoothed.ghosts), smooth)
    almost = fine_exchange(2)
    cut(first, 8, almost.faces)
    almost.post()
    corrected.forward()
    corrected.collect()

    edges = coarse_exchange(3)
    for direction in (0, 1):
        at = 3 if direction == 0 else 0
        along_rows, across_rows = pl.ds(4 * at, 4), pl.ds(at, 4, 4)
        lines = [(g, along_rows) for g in (2, 3, 4, 5)]
        lines += [(g, along_rows) for g in (0, 1)] + [(g, across_rows) for g in (4, 5)]
        lines += [(g, across_rows) for g in (0, 1, 2, 3)]
        for k, (g, rows) in enumerate(lines):
            edges.faces[direction, pl.ds(4 * k, 4), :] = corrected.ghosts[g, rows, :]
    edges.post()
    edges.near()
    for face in range(6):
        double(0, face, corrected.ghosts[face])
        own = corrected.faces[1 - face % 2, pl.ds(16 * (face // 2), 16), :]
        double(1, face, jnp.where(hop_of[face : face + 1, :] >= 0, own, 0.0))

    def lift(x, rows, outer):
        first[rows, :] = first[rows, :] + RELAX_FINE * outer

    with_ghosts(prolonged(0), lift)
    inner(first)
    almost.near()
    almost.forward()
    almost.collect()
    outermost = almost.ghosts
    own = prolonged(1)
    for face in range(6):
        outermost[face] = outermost[face] + RELAX_FINE * own(face, 0, 64)
    edges.forward()
    edges.collect()
    for face in range(6):
        double(0, face, RELAX_FINE * edges.ghosts[face])
        for k, rows in enumerate((pl.ds(0, 8), pl.ds(56, 8), pl.ds(0, 8, 8), pl.ds(7, 8, 8))):
            outermost[face, rows, :] = (
                outermost[face, rows, :] + doubled[0, face, pl.ds(8 * k, 8), :]
            )

    parts = [jnp.zeros((8, lanes), F32)] * 5

    def fold(block):
        return jnp.sum(block.reshape(8, 8, lanes), axis=0)

    def close(x, rows, outer):
        here = first[rows, :]
        applied = applied_ref[rows, :] - outer
        image[rows, :] = applied
        r = source[rows, :]
        for k, term in enumerate((r * here, here * applied, r * r, r * applied, applied * applied)):
            parts[k] = parts[k] + fold(term)

    with_ghosts(stored(outermost), close)

    tile = jnp.zeros((1, lanes), F32)
    for k in range(5):
        one = jnp.sum(jnp.sum(parts[k], axis=0, keepdims=True), axis=1, keepdims=True)
        tile = jnp.where(lane == k, one, tile)
    base = 0
    for stage, (size, mine, peer) in enumerate(stages):
        sums[base + mine] = tile
        for k in range(1, size):
            made = pltpu.make_async_remote_copy(
                src_ref=sums.at[base + mine],
                dst_ref=sums.at[base + mine],
                send_sem=sum_send.at[stage],
                recv_sem=sum_recv.at[stage],
                device_id=peer(k),
                device_id_type=MESH,
            )
            made.start()
        arriving = sums.at[pl.ds(base, size - 1)]
        for made, sends in finishing:
            if sends is None:
                made.wait_send()
            else:
                pl.when(sends)(made.wait_send)
        finishing.clear()
        pltpu.make_async_copy(arriving, arriving, sum_send.at[stage]).wait()
        pltpu.make_async_copy(arriving, arriving, sum_recv.at[stage]).wait()
        tile = jnp.sum(sums[base : base + size], axis=0)
        base += size
    tile_ref[...] = tile


def finish(p_ref, image_ref, source_ref, tile_ref, sol_hbm, res_hbm, norm_ref, sol, res, sems):
    lanes = p_ref.shape[1]
    rows_per = p_ref.shape[0] // PIECES
    lane = lax.broadcasted_iota(jnp.int32, (1, lanes), 1)
    tile = tile_ref[...]
    along, curvature, old_square, cross, image_square = [
        jnp.sum(jnp.where(lane == k, tile, 0.0), axis=1, keepdims=True) for k in range(5)
    ]
    step = along / curvature
    copies = []
    for x in range(PIECES):
        rows = pl.ds(rows_per * x, rows_per)
        sol[rows, :] = step * p_ref[rows, :]
        res[rows, :] = source_ref[rows, :] - step * image_ref[rows, :]
        for k, (here, there) in enumerate(((sol, sol_hbm), (res, res_hbm))):
            made = pltpu.make_async_copy(here.at[rows], there.at[rows], sems.at[k, x])
            made.start()
            copies.append(made)
    square = old_square - 2.0 * step * cross + step * step * image_square
    norm_ref[0] = jnp.sqrt(square)[0, 0]
    for made in copies:
        made.wait()


def local(sizes, right_side, counts, neighbours):
    cells, lanes = right_side.shape
    curve_size, level_size = sizes
    total = curve_size * level_size
    group_size = level_size * (2 - curve_size % 2)

    def body(*refs):
        curve, level = lax.axis_index("curve"), lax.axis_index("level")
        if total <= 64:
            me = curve * level_size + level

            def everyone(k):
                other = (me + k) % total
                return (other // level_size, other % level_size)

            stages = [(total, me, everyone)]
        else:
            stages = [
                (level_size, level, lambda k: (curve, (level + k) % level_size)),
                (curve_size, curve, lambda k: ((curve + k) % curve_size, level)),
            ]
        kernel(sizes, stages, group_size, *refs)

    sum_rows = total if total <= 64 else curve_size + level_size
    vmem = pl.BlockSpec(memory_space=pltpu.VMEM)
    block = jax.ShapeDtypeStruct((cells, lanes), F32)
    whole = pltpu.VMEM((cells, lanes), F32)
    out = pl.pallas_call(
        body,
        out_shape=(whole, whole, whole, pltpu.VMEM((1, lanes), F32)),
        in_specs=[pl.BlockSpec(memory_space=pl.ANY)] * 3,
        out_specs=(vmem,) * 4,
        scratch_shapes=[
            pltpu.SMEM(counts.shape, jnp.int32),
            pltpu.VMEM(neighbours.shape, jnp.int32),
            pltpu.VMEM((cells, lanes), F32),
            pltpu.VMEM((cells, lanes), F32),
            pltpu.VMEM((cells // 4, lanes), F32),
            pltpu.VMEM((2, 96, lanes), F32),
            pltpu.VMEM((cells // 8, lanes), F32),
            pltpu.VMEM((cells // 8, lanes), F32),
            pltpu.VMEM((2, 6, 32, lanes), F32),
            pltpu.VMEM((cells, lanes), F32),
            pltpu.VMEM((3, 6, 64, lanes), F32),
            pltpu.VMEM((4, 6, 16, lanes), F32),
            pltpu.VMEM((3, 2, 192, lanes), F32),
            pltpu.VMEM((3, 96, lanes), F32),
            pltpu.VMEM((3, 2, HOPS, 192, lanes), F32),
            pltpu.VMEM((4, 2, 48, lanes), F32),
            pltpu.VMEM((4, 24, lanes), F32),
            pltpu.VMEM((4, 2, HOPS, 48, lanes), F32),
            pltpu.VMEM((sum_rows, 1, lanes), F32),
            pltpu.SemaphoreType.DMA((3,)),
            pltpu.SemaphoreType.REGULAR((2, max(1, total // group_size - 1))),
            pltpu.SemaphoreType.DMA((7, 2, 3)),
            pltpu.SemaphoreType.DMA((7, 2, 3)),
            pltpu.SemaphoreType.DMA((7, 2, 3)),
            pltpu.SemaphoreType.DMA((7, 2, 3)),
            pltpu.SemaphoreType.DMA((7,)),
            pltpu.SemaphoreType.DMA((7,)),
            pltpu.SemaphoreType.DMA((7,)),
            pltpu.SemaphoreType.DMA((7,)),
            pltpu.SemaphoreType.DMA((2,)),
            pltpu.SemaphoreType.DMA((2,)),
        ],
        compiler_params=pltpu.CompilerParams(collective_id=0, has_side_effects=True),
    )(right_side, counts, neighbours)
    hbm = pl.BlockSpec(memory_space=pl.ANY)
    out = pl.pallas_call(
        finish,
        out_shape=(block, block, jax.ShapeDtypeStruct((1,), F32)),
        in_specs=[vmem] * 4,
        out_specs=(hbm, hbm, pl.BlockSpec(memory_space=pltpu.SMEM)),
        scratch_shapes=[
            pltpu.VMEM((cells, lanes), F32),
            pltpu.VMEM((cells, lanes), F32),
            pltpu.SemaphoreType.DMA((2, PIECES)),
        ],
    )(*[pltpu.with_memory_space_constraint(a, pltpu.VMEM) for a in out])
    return out[0], out[1], out[2].reshape(())


def solution(mesh):
    sizes = tuple(mesh.shape[name] for name in AXES)
    in_specs = (P(None, AXES), P(), P(None, AXES))
    out_specs = (P(None, AXES), P(None, AXES), P())
    return jax.shard_map(
        functools.partial(local, sizes), mesh=mesh, in_specs=in_specs, out_specs=out_specs, check_vma=False
    )
```

```python
import functools

import jax
import jax.numpy as jnp
from jax import lax
from jax.experimental import pallas as pl
from jax.experimental.pallas import tpu as pltpu
from jax.sharding import PartitionSpec as P

MIN_LIVE = 96
LAYER = 256
HOPS = 3
PIECES = 2
AXES = ("curve", "level")
MESH = pl.DeviceIdType.MESH
RELAXATION = 2.0 / 3.0
RELAX_FINE = RELAXATION / 6.0
RELAX_COARSE = RELAXATION / 1.5
F32 = jnp.float32


def kernel(
    sizes,
    stages,
    group_size,
    right_hbm,
    counts_hbm,
    neighbours_hbm,
    first,
    image,
    source,
    tile_ref,
    counts_ref,
    neighbours_ref,
    second,
    zghost,
    paired,
    halved,
    yghost_coarse,
    zghost_coarse,
    doubled,
    applied_ref,
    ghosts_fine,
    ghosts_coarse,
    faces_fine,
    packed_fine,
    windows_fine,
    faces_coarse,
    packed_coarse,
    windows_coarse,
    sums,
    loads,
    words,
    *sems,
):
    link_sems, relay_sems, pair_sems, far_sems, (sum_send, sum_recv) = [
        sems[i : i + 2] for i in range(0, 10, 2)
    ]
    curve_size, level_size = sizes
    total = curve_size * level_size
    me = lax.axis_index("curve") * level_size + lax.axis_index("level")
    lanes = source.shape[1]
    half = lanes // 2

    def place(index):
        return (index // level_size, index % level_size)

    inputs = [
        pltpu.make_async_copy(src, dst, loads.at[k])
        for k, (src, dst) in enumerate(
            ((right_hbm, second), (counts_hbm, counts_ref), (neighbours_hbm, neighbours_ref))
        )
    ]
    for made in inputs:
        made.start()
    barrier = pltpu.get_barrier_semaphore()
    greeted = 0
    groups = total // group_size
    group = me // group_size
    if len(stages) > 1:
        for hop in range(1, HOPS + 1):
            for sign in (1, -1):
                target = (me + sign * hop + total) % total
                pl.semaphore_signal(barrier, inc=1, device_id=place(target), device_id_type=MESH)
                greeted += 1
        for size, _, peer in stages:
            for k in range(1, size):
                pl.semaphore_signal(barrier, inc=1, device_id=peer(k), device_id_type=MESH)
                greeted += 1
    else:
        for hop in sorted({*range(1, HOPS + 1), *range(1, group_size + 1)}):
            for sign in (1, -1):
                target = me + sign * hop
                there = (target >= 0) & (target < total)
                if HOPS < hop < group_size:
                    there = there & ((target + total) // group_size == group + groups)

                @pl.when(there)
                def _():
                    pl.semaphore_signal(
                        barrier,
                        inc=1,
                        device_id=place((target + total) % total),
                        device_id_type=MESH,
                    )

                greeted = greeted + there.astype(jnp.int32)

    def pass_word(step):
        if len(stages) > 1 or step > groups:
            return
        sides = ((0, 1, group), (1, -1, groups - 1 - group))
        if step > 1:
            for side, _, known in sides:

                @pl.when(known >= step - 1)
                def _():
                    pl.semaphore_wait(words.at[side, step - 2], 1)

        if step < groups:
            for side, sign, known in sides:
                target = me + sign * group_size

                @pl.when((known >= step - 1) & (target >= 0) & (target < total))
                def _():
                    pl.semaphore_signal(
                        words.at[side, step - 1],
                        inc=1,
                        device_id=place((target + total) % total),
                        device_id_type=MESH,
                    )

    zghost[...] = jnp.zeros_like(zghost)
    yghost_coarse[...] = jnp.zeros_like(yghost_coarse)
    zghost_coarse[...] = jnp.zeros_like(zghost_coarse)
    for made in inputs:
        made.wait()

    lane = lax.broadcasted_iota(jnp.int32, (1, lanes), 1)
    own_count = counts_ref[me]
    live = lane < own_count
    for x in range(8):
        rows = pl.ds(64 * x, 64)
        value = jnp.where(live, second[rows, :], 0.0)
        source[rows, :] = value
        first[rows, :] = RELAX_FINE * value

    nb = neighbours_ref[...]
    present = nb >= 0
    owner = nb // lanes
    offset = nb % lanes
    face_id = lax.broadcasted_iota(jnp.int32, nb.shape, 0)
    hop_of = jnp.where(face_id % 2 == 0, me - owner, owner - me)
    hop_of = jnp.where(present, hop_of, -1)
    far_count = counts_ref[jnp.maximum(me - HOPS, 0)]
    odd = me % 2
    even = 1 - odd
    partner = me + 1 - 2 * odd
    earlier_pair = me >= 2
    later_pair = me - odd + 2 < total
    reaches = (1 + 2 * even, 1 + 2 * odd)
    arrives = (2 * odd, 2 * even)
    far_there = jnp.where(odd == 1, me + HOPS < total, me >= HOPS)
    far_device = (me + HOPS * (2 * odd - 1) + total) % total
    skipped = jnp.where(
        (face_id % 2 == 0) & (hop_of == HOPS), even * (far_count - half), 0
    )
    where_at = jnp.clip(offset - skipped, 0, lanes - 1)
    skipped = jnp.where((face_id % 2 == 0) & (hop_of == HOPS), far_count - half, 0)
    where_direct = jnp.clip(offset - skipped, 0, lanes - 1)
    near_index = jnp.broadcast_to(lane % half, (8, lanes))
    last_index = near_index + (own_count - half)
    low_half = jnp.broadcast_to(lane < half, (8, lanes))
    pack_index = jnp.broadcast_to(odd * (own_count - half) + lane % half, (8, lanes))

    def pick(block, index):
        return jnp.take_along_axis(block, index, axis=1, mode="promise_in_bounds")

    finishing = []

    def send(src, dst, sems, at, target, sends):
        made = pltpu.make_async_remote_copy(
            src_ref=src,
            dst_ref=dst,
            send_sem=sems[0].at[at],
            recv_sem=sems[1].at[at],
            device_id=place(target),
            device_id_type=MESH,
        )
        finishing.append((made, sends))
        return made

    def cut(values, extent, faces):
        area = extent * extent
        for direction in (0, 1):
            at = extent - 1 if direction == 0 else 0
            faces[direction, 0:area, :] = values[pl.ds(at * area, area), :]
            for x in range(extent):
                faces[direction, pl.ds(area + x * extent, extent), :] = values[
                    pl.ds(x * area + at * extent, extent), :
                ]
            faces[direction, pl.ds(2 * area, area), :] = values[pl.ds(at, area, extent), :]

    class Exchange:
        def __init__(self, stage, area, chunks, faces, packed, windows, ghosts):
            self.stage, self.area, self.chunks = stage, area, chunks
            self.faces, self.packed, self.windows, self.ghosts = faces, packed, windows, ghosts

        def post(self):
            faces, packed, windows, stage = self.faces, self.packed, self.windows, self.stage
            size = 3 * self.area // self.chunks
            pack = 3 * self.area // 2
            self.links = []
            for chunk in range(self.chunks):
                rows = pl.ds(chunk * size, size)
                for direction in (0, 1):
                    reach = reaches[direction]
                    target = me + reach if direction == 0 else me - reach
                    made = send(
                        faces.at[direction, rows],
                        windows.at[direction, reach - 1, rows],
                        link_sems,
                        (stage, direction, chunk),
                        (target + total) % total,
                        later_pair if direction == 0 else earlier_pair,
                    )
                    pl.when(later_pair if direction == 0 else earlier_pair)(made.start)
                    self.links.append((direction, chunk, rows, made))
            self.inside = send(
                faces.at[odd], windows.at[odd, 0], pair_sems, (stage,), partner, None
            )
            self.inside.start()
            for r in range(0, pack, 8):
                a = pick(faces[1 - odd, pl.ds(r, 8), :], pack_index)
                b = pick(faces[1 - odd, pl.ds(pack + r, 8), :], pack_index)
                packed[pl.ds(r, 8), :] = jnp.where(low_half, a, b)
            self.far = send(
                packed,
                windows.at[1 - odd, 2, pl.ds(0, pack)],
                far_sems,
                (stage,),
                far_device,
                far_there,
            )
            pl.when(far_there)(self.far.start)

        def pull(self, face, hops_in):
            area, faces, windows = self.area, self.faces, self.windows
            pack = 3 * area // 2
            direction, slot = face % 2, face // 2
            at = jnp.broadcast_to(where_at[face : face + 1, :], (8, lanes))
            is_packed = odd == direction
            at_high = jnp.where(is_packed, jnp.minimum(at + half, lanes - 1), at)
            hops = jnp.broadcast_to(hop_of[face : face + 1, :], (8, lanes))
            for r in range(0, area, 8):
                row = slot * area + r
                if 0 in hops_in:
                    block = jnp.zeros((8, lanes), F32)
                else:
                    block = self.ghosts[face, pl.ds(r, 8), :]
                for hop in hops_in:
                    index = at
                    if hop == 0:
                        window = faces[direction, pl.ds(row, 8), :]
                    elif hop < HOPS or row < pack:
                        window = windows[direction, hop - 1, pl.ds(row, 8), :]
                    else:
                        start = pl.multiple_of(row - jnp.where(is_packed, pack, 0), 8)
                        window = windows[direction, hop - 1, pl.ds(start, 8), :]
                        index = at_high
                    block = jnp.where(hops == hop, pick(window, index), block)
                self.ghosts[face, pl.ds(r, 8), :] = block

        def near(self):
            for face in range(6):
                self.pull(face, (0,))

        def forward(self):
            self.relays = {}
            for direction, chunk, rows, made in self.links:
                comes = earlier_pair if direction == 0 else later_pair
                relay = send(
                    self.windows.at[direction, arrives[direction], rows],
                    self.windows.at[direction, 1, rows],
                    relay_sems,
                    (self.stage, direction, chunk),
                    partner,
                    comes,
                )

                @pl.when(comes)
                def _():
                    made.wait_recv()
                    relay.start()

                self.relays[direction, chunk] = (relay, comes)

        def collect(self):
            self.inside.wait_recv()
            pl.when(far_there)(self.far.wait_recv)
            for face in range(6):
                waits = self.relays.pop((face % 2, face // 2), None)
                if waits is not None:
                    relay, comes = waits
                    pl.when(comes)(relay.wait_recv)
                self.pull(face, (1, 2, 3))

    class Direct(Exchange):
        def post(self):
            faces, packed, windows, stage = self.faces, self.packed, self.windows, self.stage
            pack = 3 * self.area // 2
            self.links = []

            def start(hop, direction, src, dst):
                target = me + hop if direction == 0 else me - hop
                source_at = me - hop if direction == 0 else me + hop
                there = (target >= 0) & (target < total)
                comes = (source_at >= 0) & (source_at < total)
                at = (stage, direction, hop - 1)
                made = send(src, dst, link_sems, at, (target + total) % total, there)
                pl.when(there)(made.start)
                self.links.append((made, comes))

            for hop in (3, 2, 1):
                for direction in (0, 1):
                    if hop < HOPS:
                        start(hop, direction, faces.at[direction], windows.at[direction, hop - 1])
                        continue
                    index = last_index if direction == 0 else near_index
                    for r in range(0, pack, 8):
                        a = pick(faces[direction, pl.ds(r, 8), :], index)
                        b = pick(faces[direction, pl.ds(pack + r, 8), :], index)
                        packed[direction, pl.ds(r, 8), :] = jnp.where(low_half, a, b)
                    start(
                        hop,
                        direction,
                        packed.at[direction],
                        windows.at[direction, hop - 1, pl.ds(0, pack)],
                    )

        def pull(self, face, hops_in):
            area, faces, windows = self.area, self.faces, self.windows
            pack = 3 * area // 2
            direction, slot = face % 2, face // 2
            at = jnp.broadcast_to(where_direct[face : face + 1, :], (8, lanes))
            at_high = jnp.minimum(at + half, lanes - 1)
            hops = jnp.broadcast_to(hop_of[face : face + 1, :], (8, lanes))
            for r in range(0, area, 8):
                row = slot * area + r
                if 0 in hops_in:
                    block = jnp.zeros((8, lanes), F32)
                else:
                    block = self.ghosts[face, pl.ds(r, 8), :]
                for hop in hops_in:
                    if hop == 0:
                        moved = pick(faces[direction, pl.ds(row, 8), :], at)
                    elif hop < HOPS:
                        moved = pick(windows[direction, hop - 1, pl.ds(row, 8), :], at)
                    else:
                        window = windows[direction, hop - 1, pl.ds(row % pack, 8), :]
                        moved = pick(window, at if row < pack else at_high)
                    block = jnp.where(hops == hop, moved, block)
                self.ghosts[face, pl.ds(r, 8), :] = block

        def forward(self):
            pass

        def collect(self):
            for made, comes in self.links:
                pl.when(comes)(made.wait_recv)
            for face in range(6):
                self.pull(face, (1, 2, 3))

    def fine_exchange(k):
        return Exchange(
            k, 64, 3, faces_fine.at[k], packed_fine.at[k], windows_fine.at[k], ghosts_fine.at[k]
        )

    def coarse_exchange(k):
        kind = Direct if k in (1, 3) else Exchange
        packed = packed_coarse.at[k]
        return kind(
            3 + k,
            16,
            1,
            faces_coarse.at[k],
            packed if k in (1, 3) else packed.at[0],
            windows_coarse.at[k],
            ghosts_coarse.at[k],
        )

    zrow = lax.broadcasted_iota(jnp.int32, (8, 8, lanes), 1)

    def inner(values):
        for x in range(8):
            rows = pl.ds(64 * x, 64)
            here = values[rows, :]
            edge = jnp.zeros((8, lanes), F32)
            beside = jnp.concatenate([edge, here[:-8]], axis=0) + jnp.concatenate(
                [here[8:], edge], axis=0
            )
            if x > 0:
                beside = beside + values[pl.ds(64 * (x - 1), 64), :]
            if x < 7:
                beside = beside + values[pl.ds(64 * (x + 1), 64), :]
            cube = here.reshape(8, 8, lanes)
            below = jnp.where(zrow == 0, 0.0, pltpu.roll(cube, 1, 1))
            above = jnp.where(zrow == 7, 0.0, pltpu.roll(cube, 7, 1))
            beside = beside + (below + above).reshape(64, lanes)
            applied_ref[rows, :] = 6.0 * here - beside

    def with_ghosts(ghost, use):
        zghost[pl.ds(0, 64, 8), :] = ghost(4, 0, 64)
        zghost[pl.ds(7, 64, 8), :] = ghost(5, 0, 64)
        for x in range(8):
            rows = pl.ds(64 * x, 64)
            outer = zghost[rows, :]
            if x == 0:
                outer = outer + ghost(0, 0, 64)
            if x == 7:
                outer = outer + ghost(1, 0, 64)
            outer = jnp.concatenate(
                [
                    outer[:8] + ghost(2, 8 * x, 8),
                    outer[8:56],
                    outer[56:] + ghost(3, 8 * x, 8),
                ],
                axis=0,
            )
            use(x, rows, outer)

    def stored(ghosts):
        return lambda face, start, size: ghosts[face, pl.ds(start, size), :]

    def prolonged(k):
        def ghost(face, start, size):
            return jnp.concatenate(
                [
                    doubled[k, face, pl.ds(8 * (a // 2), 8), :]
                    for a in range(start // 8, (start + size) // 8)
                ],
                axis=0,
            )

        return ghost

    def double(k, face, value):
        doubled[k, face, pl.ds(0, 16, 2), :] = value
        doubled[k, face, pl.ds(1, 16, 2), :] = value

    def coarse_outer(ghosts):
        zghost_coarse[pl.ds(0, 16, 4), :] = ghosts[4]
        zghost_coarse[pl.ds(3, 16, 4), :] = ghosts[5]
        for x in range(4):
            yghost_coarse[pl.ds(16 * x, 4), :] = ghosts[2, pl.ds(4 * x, 4), :]
            yghost_coarse[pl.ds(16 * x + 12, 4), :] = ghosts[3, pl.ds(4 * x, 4), :]
        outer = yghost_coarse[...] + zghost_coarse[...]
        return jnp.concatenate(
            [outer[:16] + ghosts[0], outer[16:48], outer[48:] + ghosts[1]], axis=0
        )

    exchange = fine_exchange(0)
    cut(first, 8, exchange.faces)
    pl.semaphore_wait(barrier, greeted)
    exchange.post()
    pass_word(1)
    exchange.near()
    inner(first)
    exchange.forward()
    pass_word(2)
    exchange.collect()

    def sweep(x, rows, outer):
        second[rows, :] = first[rows, :] + RELAX_FINE * (
            source[rows, :] - applied_ref[rows, :] + outer
        )

    with_ghosts(stored(exchange.ghosts), sweep)

    smoothed = fine_exchange(1)
    sampled = coarse_exchange(0)
    cut(second, 8, smoothed.faces)
    for direction in (0, 1):
        for k in range(12):
            halved[direction, pl.ds(8 * k, 8), :] = (
                smoothed.faces[direction, pl.ds(16 * k, 8), :]
                + smoothed.faces[direction, pl.ds(16 * k + 8, 8), :]
            )
        sampled.faces[direction, :, :] = (
            halved[direction, pl.ds(0, 48, 2), :] + halved[direction, pl.ds(1, 48, 2), :]
        )
    sampled.post()
    smoothed.post()
    sampled.near()
    inner(second)
    for x in range(0, 8, 2):
        lower, upper = pl.ds(64 * x, 64), pl.ds(64 * x + 64, 64)
        both = (source[lower, :] - applied_ref[lower, :]) + (
            source[upper, :] - applied_ref[upper, :]
        )
        for y in range(4):
            paired[pl.ds(32 * (x // 2) + 8 * y, 8), :] = (
                both[16 * y : 16 * y + 8] + both[16 * y + 8 : 16 * y + 16]
            )
    inner_rhs = paired[pl.ds(0, 64, 2), :] + paired[pl.ds(1, 64, 2), :]
    smoothed.near()
    sampled.forward()
    pass_word(3)
    sampled.collect()
    coarse_rhs = 0.125 * (inner_rhs + coarse_outer(sampled.ghosts))
    coarse_one = RELAX_COARSE * coarse_rhs

    exchange = coarse_exchange(1)
    coarse = halved.at[0]
    coarse[0:64, :] = coarse_one
    cut(coarse, 4, exchange.faces)
    exchange.post()
    exchange.near()
    row = lax.broadcasted_iota(jnp.int32, (64, lanes), 0)
    edge = jnp.zeros((16, lanes), F32)
    beside = jnp.concatenate([edge, coarse_one[:-16]], axis=0) + jnp.concatenate(
        [coarse_one[16:], edge], axis=0
    )
    beside = beside + jnp.where(row // 4 % 4 == 0, 0.0, pltpu.roll(coarse_one, 4, 0))
    beside = beside + jnp.where(row // 4 % 4 == 3, 0.0, pltpu.roll(coarse_one, 60, 0))
    beside = beside + jnp.where(row % 4 == 0, 0.0, pltpu.roll(coarse_one, 1, 0))
    beside = beside + jnp.where(row % 4 == 3, 0.0, pltpu.roll(coarse_one, 63, 0))
    coarse_two = coarse_one + RELAX_COARSE * (coarse_rhs - 0.25 * (6.0 * coarse_one - beside))
    smoothed.forward()
    exchange.forward()
    for step in range(4, total // group_size + 1):
        pass_word(step)
    exchange.collect()
    coarse_two = coarse_two + (0.25 * RELAX_COARSE) * coarse_outer(exchange.ghosts)

    corrected = coarse_exchange(2)
    coarse[0:64, :] = coarse_two
    cut(coarse, 4, corrected.faces)
    corrected.post()
    corrected.near()
    paired[pl.ds(0, 64, 2), :] = coarse_two
    paired[pl.ds(1, 64, 2), :] = coarse_two
    for x in range(8):
        for y in range(8):
            rows = pl.ds(64 * x + 8 * y, 8)
            lift = paired[pl.ds(32 * (x // 2) + 8 * (y // 2), 8), :]
            second[rows, :] = second[rows, :] + lift
    inner(second)
    smoothed.collect()

    def smooth(x, rows, outer):
        first[rows, :] = second[rows, :] + RELAX_FINE * (
            source[rows, :] - applied_ref[rows, :] + outer
        )

    with_ghosts(stored(smoothed.ghosts), smooth)
    almost = fine_exchange(2)
    cut(first, 8, almost.faces)
    almost.post()
    corrected.forward()
    corrected.collect()

    edges = coarse_exchange(3)
    for direction in (0, 1):
        at = 3 if direction == 0 else 0
        along_rows, across_rows = pl.ds(4 * at, 4), pl.ds(at, 4, 4)
        lines = [(g, along_rows) for g in (2, 3, 4, 5)]
        lines += [(g, along_rows) for g in (0, 1)] + [(g, across_rows) for g in (4, 5)]
        lines += [(g, across_rows) for g in (0, 1, 2, 3)]
        for k, (g, rows) in enumerate(lines):
            edges.faces[direction, pl.ds(4 * k, 4), :] = corrected.ghosts[g, rows, :]
    edges.post()
    edges.near()
    for face in range(6):
        double(0, face, corrected.ghosts[face])
        own = corrected.faces[1 - face % 2, pl.ds(16 * (face // 2), 16), :]
        double(1, face, jnp.where(hop_of[face : face + 1, :] >= 0, own, 0.0))

    def lift(x, rows, outer):
        first[rows, :] = first[rows, :] + RELAX_FINE * outer

    with_ghosts(prolonged(0), lift)
    inner(first)
    almost.near()
    almost.forward()
    almost.collect()
    outermost = almost.ghosts
    own = prolonged(1)
    for face in range(6):
        outermost[face] = outermost[face] + RELAX_FINE * own(face, 0, 64)
    edges.forward()
    edges.collect()
    for face in range(6):
        double(0, face, RELAX_FINE * edges.ghosts[face])
        for k, rows in enumerate((pl.ds(0, 8), pl.ds(56, 8), pl.ds(0, 8, 8), pl.ds(7, 8, 8))):
            outermost[face, rows, :] = (
                outermost[face, rows, :] + doubled[0, face, pl.ds(8 * k, 8), :]
            )

    parts = [jnp.zeros((8, lanes), F32)] * 5

    def fold(block):
        return jnp.sum(block.reshape(8, 8, lanes), axis=0)

    def close(x, rows, outer):
        here = first[rows, :]
        applied = applied_ref[rows, :] - outer
        image[rows, :] = applied
        r = source[rows, :]
        for k, term in enumerate((r * here, here * applied, r * r, r * applied, applied * applied)):
            parts[k] = parts[k] + fold(term)

    with_ghosts(stored(outermost), close)

    tile = jnp.zeros((1, lanes), F32)
    for k in range(5):
        one = jnp.sum(jnp.sum(parts[k], axis=0, keepdims=True), axis=1, keepdims=True)
        tile = jnp.where(lane == k, one, tile)
    base = 0
    for stage, (size, mine, peer) in enumerate(stages):
        sums[base + mine] = tile
        for k in range(1, size):
            made = pltpu.make_async_remote_copy(
                src_ref=sums.at[base + mine],
                dst_ref=sums.at[base + mine],
                send_sem=sum_send.at[stage],
                recv_sem=sum_recv.at[stage],
                device_id=peer(k),
                device_id_type=MESH,
            )
            made.start()
        arriving = sums.at[pl.ds(base, size - 1)]
        for made, sends in finishing:
            if sends is None:
                made.wait_send()
            else:
                pl.when(sends)(made.wait_send)
        finishing.clear()
        pltpu.make_async_copy(arriving, arriving, sum_send.at[stage]).wait()
        pltpu.make_async_copy(arriving, arriving, sum_recv.at[stage]).wait()
        tile = jnp.sum(sums[base : base + size], axis=0)
        base += size
    tile_ref[...] = tile


def finish(p_ref, image_ref, source_ref, tile_ref, sol_hbm, res_hbm, norm_ref, sol, res, sems):
    lanes = p_ref.shape[1]
    rows_per = p_ref.shape[0] // PIECES
    lane = lax.broadcasted_iota(jnp.int32, (1, lanes), 1)
    tile = tile_ref[...]
    along, curvature, old_square, cross, image_square = [
        jnp.sum(jnp.where(lane == k, tile, 0.0), axis=1, keepdims=True) for k in range(5)
    ]
    step = along / curvature
    copies = []
    for x in range(PIECES):
        rows = pl.ds(rows_per * x, rows_per)
        sol[rows, :] = step * p_ref[rows, :]
        res[rows, :] = source_ref[rows, :] - step * image_ref[rows, :]
        for k, (here, there) in enumerate(((sol, sol_hbm), (res, res_hbm))):
            made = pltpu.make_async_copy(here.at[rows], there.at[rows], sems.at[k, x])
            made.start()
            copies.append(made)
    square = old_square - 2.0 * step * cross + step * step * image_square
    norm_ref[0] = jnp.sqrt(square)[0, 0]
    for made in copies:
        made.wait()


def local(sizes, right_side, counts, neighbours):
    cells, lanes = right_side.shape
    curve_size, level_size = sizes
    total = curve_size * level_size
    group_size = level_size * (2 - curve_size % 2)

    def body(*refs):
        curve, level = lax.axis_index("curve"), lax.axis_index("level")
        if total <= 64:
            me = curve * level_size + level

            def everyone(k):
                other = (me + k) % total
                return (other // level_size, other % level_size)

            stages = [(total, me, everyone)]
        else:
            stages = [
                (level_size, level, lambda k: (curve, (level + k) % level_size)),
                (curve_size, curve, lambda k: ((curve + k) % curve_size, level)),
            ]
        kernel(sizes, stages, group_size, *refs)

    sum_rows = total if total <= 64 else curve_size + level_size
    vmem = pl.BlockSpec(memory_space=pltpu.VMEM)
    block = jax.ShapeDtypeStruct((cells, lanes), F32)
    whole = pltpu.VMEM((cells, lanes), F32)
    out = pl.pallas_call(
        body,
        out_shape=(whole, whole, whole, pltpu.VMEM((1, lanes), F32)),
        in_specs=[pl.BlockSpec(memory_space=pl.ANY)] * 3,
        out_specs=(vmem,) * 4,
        scratch_shapes=[
            pltpu.SMEM(counts.shape, jnp.int32),
            pltpu.VMEM(neighbours.shape, jnp.int32),
            pltpu.VMEM((cells, lanes), F32),
            pltpu.VMEM((cells, lanes), F32),
            pltpu.VMEM((cells // 4, lanes), F32),
            pltpu.VMEM((2, 96, lanes), F32),
            pltpu.VMEM((cells // 8, lanes), F32),
            pltpu.VMEM((cells // 8, lanes), F32),
            pltpu.VMEM((2, 6, 32, lanes), F32),
            pltpu.VMEM((cells, lanes), F32),
            pltpu.VMEM((3, 6, 64, lanes), F32),
            pltpu.VMEM((4, 6, 16, lanes), F32),
            pltpu.VMEM((3, 2, 192, lanes), F32),
            pltpu.VMEM((3, 96, lanes), F32),
            pltpu.VMEM((3, 2, HOPS, 192, lanes), F32),
            pltpu.VMEM((4, 2, 48, lanes), F32),
            pltpu.VMEM((4, 2, 24, lanes), F32),
            pltpu.VMEM((4, 2, HOPS, 48, lanes), F32),
            pltpu.VMEM((sum_rows, 1, lanes), F32),
            pltpu.SemaphoreType.DMA((3,)),
            pltpu.SemaphoreType.REGULAR((2, max(1, total // group_size - 1))),
            pltpu.SemaphoreType.DMA((7, 2, 3)),
            pltpu.SemaphoreType.DMA((7, 2, 3)),
            pltpu.SemaphoreType.DMA((7, 2, 3)),
            pltpu.SemaphoreType.DMA((7, 2, 3)),
            pltpu.SemaphoreType.DMA((7,)),
            pltpu.SemaphoreType.DMA((7,)),
            pltpu.SemaphoreType.DMA((7,)),
            pltpu.SemaphoreType.DMA((7,)),
            pltpu.SemaphoreType.DMA((2,)),
            pltpu.SemaphoreType.DMA((2,)),
        ],
        compiler_params=pltpu.CompilerParams(collective_id=0, has_side_effects=True),
    )(right_side, counts, neighbours)
    hbm = pl.BlockSpec(memory_space=pl.ANY)
    out = pl.pallas_call(
        finish,
        out_shape=(block, block, jax.ShapeDtypeStruct((1,), F32)),
        in_specs=[vmem] * 4,
        out_specs=(hbm, hbm, pl.BlockSpec(memory_space=pltpu.SMEM)),
        scratch_shapes=[
            pltpu.VMEM((cells, lanes), F32),
            pltpu.VMEM((cells, lanes), F32),
            pltpu.SemaphoreType.DMA((2, PIECES)),
        ],
    )(*[pltpu.with_memory_space_constraint(a, pltpu.VMEM) for a in out])
    return out[0], out[1], out[2].reshape(())


def solution(mesh):
    sizes = tuple(mesh.shape[name] for name in AXES)
    in_specs = (P(None, AXES), P(), P(None, AXES))
    out_specs = (P(None, AXES), P(None, AXES), P())
    return jax.shard_map(
        functools.partial(local, sizes), mesh=mesh, in_specs=in_specs, out_specs=out_specs, check_vma=False
    )
```

```python
import functools

import jax
import jax.numpy as jnp
from jax import lax
from jax.experimental import pallas as pl
from jax.experimental.pallas import tpu as pltpu
from jax.sharding import PartitionSpec as P

MIN_LIVE = 96
LAYER = 256
HOPS = 3
PIECES = 2
AXES = ("curve", "level")
MESH = pl.DeviceIdType.MESH
RELAXATION = 2.0 / 3.0
RELAX_FINE = RELAXATION / 6.0
RELAX_COARSE = RELAXATION / 1.5
F32 = jnp.float32


def kernel(
    sizes,
    stages,
    group_size,
    right_hbm,
    counts_hbm,
    neighbours_hbm,
    first,
    image,
    source,
    tile_ref,
    counts_ref,
    neighbours_ref,
    second,
    zghost,
    paired,
    halved,
    yghost_coarse,
    zghost_coarse,
    doubled,
    applied_ref,
    ghosts_fine,
    ghosts_coarse,
    faces_fine,
    packed_fine,
    windows_fine,
    faces_coarse,
    packed_coarse,
    windows_coarse,
    sums,
    loads,
    words,
    *sems,
):
    link_sems, relay_sems, pair_sems, far_sems, (sum_send, sum_recv) = [
        sems[i : i + 2] for i in range(0, 10, 2)
    ]
    curve_size, level_size = sizes
    total = curve_size * level_size
    me = lax.axis_index("curve") * level_size + lax.axis_index("level")
    lanes = source.shape[1]
    half = lanes // 2

    def place(index):
        return (index // level_size, index % level_size)

    inputs = [
        pltpu.make_async_copy(src, dst, loads.at[k])
        for k, (src, dst) in enumerate(
            ((right_hbm, second), (counts_hbm, counts_ref), (neighbours_hbm, neighbours_ref))
        )
    ]
    for made in inputs:
        made.start()
    barrier = pltpu.get_barrier_semaphore()
    greeted = 0
    groups = total // group_size
    group = me // group_size
    if len(stages) > 1:
        for hop in range(1, HOPS + 1):
            for sign in (1, -1):
                target = (me + sign * hop + total) % total
                pl.semaphore_signal(barrier, inc=1, device_id=place(target), device_id_type=MESH)
                greeted += 1
        for size, _, peer in stages:
            for k in range(1, size):
                pl.semaphore_signal(barrier, inc=1, device_id=peer(k), device_id_type=MESH)
                greeted += 1
    else:
        for hop in sorted({*range(1, HOPS + 1), *range(1, group_size + 1)}):
            for sign in (1, -1):
                target = me + sign * hop
                there = (target >= 0) & (target < total)
                if HOPS < hop < group_size:
                    there = there & ((target + total) // group_size == group + groups)

                @pl.when(there)
                def _():
                    pl.semaphore_signal(
                        barrier,
                        inc=1,
                        device_id=place((target + total) % total),
                        device_id_type=MESH,
                    )

                greeted = greeted + there.astype(jnp.int32)

    def pass_word(step):
        if len(stages) > 1 or step > groups:
            return
        sides = ((0, 1, group), (1, -1, groups - 1 - group))
        if step > 1:
            for side, _, known in sides:

                @pl.when(known >= step - 1)
                def _():
                    pl.semaphore_wait(words.at[side, step - 2], 1)

        if step < groups:
            for side, sign, known in sides:
                target = me + sign * group_size

                @pl.when((known >= step - 1) & (target >= 0) & (target < total))
                def _():
                    pl.semaphore_signal(
                        words.at[side, step - 1],
                        inc=1,
                        device_id=place((target + total) % total),
                        device_id_type=MESH,
                    )

    zghost[...] = jnp.zeros_like(zghost)
    yghost_coarse[...] = jnp.zeros_like(yghost_coarse)
    zghost_coarse[...] = jnp.zeros_like(zghost_coarse)
    for made in inputs:
        made.wait()

    lane = lax.broadcasted_iota(jnp.int32, (1, lanes), 1)
    own_count = counts_ref[me]
    live = lane < own_count
    for x in range(8):
        rows = pl.ds(64 * x, 64)
        value = jnp.where(live, second[rows, :], 0.0)
        source[rows, :] = value
        first[rows, :] = RELAX_FINE * value

    nb = neighbours_ref[...]
    present = nb >= 0
    owner = nb // lanes
    offset = nb % lanes
    face_id = lax.broadcasted_iota(jnp.int32, nb.shape, 0)
    hop_of = jnp.where(face_id % 2 == 0, me - owner, owner - me)
    hop_of = jnp.where(present, hop_of, -1)
    far_count = counts_ref[jnp.maximum(me - HOPS, 0)]
    odd = me % 2
    even = 1 - odd
    partner = me + 1 - 2 * odd
    earlier_pair = me >= 2
    later_pair = me - odd + 2 < total
    reaches = (1 + 2 * even, 1 + 2 * odd)
    arrives = (2 * odd, 2 * even)
    far_there = jnp.where(odd == 1, me + HOPS < total, me >= HOPS)
    far_device = (me + HOPS * (2 * odd - 1) + total) % total
    skipped = jnp.where(
        (face_id % 2 == 0) & (hop_of == HOPS), even * (far_count - half), 0
    )
    where_at = jnp.clip(offset - skipped, 0, lanes - 1)
    skipped = jnp.where((face_id % 2 == 0) & (hop_of == HOPS), far_count - half, 0)
    where_direct = jnp.clip(offset - skipped, 0, lanes - 1)
    near_index = jnp.broadcast_to(lane % half, (8, lanes))
    last_index = near_index + (own_count - half)
    low_half = jnp.broadcast_to(lane < half, (8, lanes))
    pack_index = jnp.broadcast_to(odd * (own_count - half) + lane % half, (8, lanes))

    def pick(block, index):
        return jnp.take_along_axis(block, index, axis=1, mode="promise_in_bounds")

    finishing = []

    def send(src, dst, sems, at, target, sends):
        made = pltpu.make_async_remote_copy(
            src_ref=src,
            dst_ref=dst,
            send_sem=sems[0].at[at],
            recv_sem=sems[1].at[at],
            device_id=place(target),
            device_id_type=MESH,
        )
        finishing.append((made, sends))
        return made

    def cut(values, extent, faces):
        area = extent * extent
        for direction in (0, 1):
            at = extent - 1 if direction == 0 else 0
            faces[direction, 0:area, :] = values[pl.ds(at * area, area), :]
            for x in range(extent):
                faces[direction, pl.ds(area + x * extent, extent), :] = values[
                    pl.ds(x * area + at * extent, extent), :
                ]
            faces[direction, pl.ds(2 * area, area), :] = values[pl.ds(at, area, extent), :]

    class Exchange:
        def __init__(self, stage, area, chunks, faces, packed, windows, ghosts):
            self.stage, self.area, self.chunks = stage, area, chunks
            self.faces, self.packed, self.windows, self.ghosts = faces, packed, windows, ghosts

        def post(self):
            faces, packed, windows, stage = self.faces, self.packed, self.windows, self.stage
            size = 3 * self.area // self.chunks
            pack = 3 * self.area // 2
            self.links = []
            for chunk in range(self.chunks):
                rows = pl.ds(chunk * size, size)
                for direction in (0, 1):
                    reach = reaches[direction]
                    target = me + reach if direction == 0 else me - reach
                    made = send(
                        faces.at[direction, rows],
                        windows.at[direction, reach - 1, rows],
                        link_sems,
                        (stage, direction, chunk),
                        (target + total) % total,
                        later_pair if direction == 0 else earlier_pair,
                    )
                    pl.when(later_pair if direction == 0 else earlier_pair)(made.start)
                    self.links.append((direction, chunk, rows, made))
            self.inside = send(
                faces.at[odd], windows.at[odd, 0], pair_sems, (stage,), partner, None
            )
            self.inside.start()
            for r in range(0, pack, 8):
                a = pick(faces[1 - odd, pl.ds(r, 8), :], pack_index)
                b = pick(faces[1 - odd, pl.ds(pack + r, 8), :], pack_index)
                packed[pl.ds(r, 8), :] = jnp.where(low_half, a, b)
            self.far = send(
                packed,
                windows.at[1 - odd, 2, pl.ds(0, pack)],
                far_sems,
                (stage,),
                far_device,
                far_there,
            )
            pl.when(far_there)(self.far.start)

        def pull(self, face, hops_in):
            area, faces, windows = self.area, self.faces, self.windows
            pack = 3 * area // 2
            direction, slot = face % 2, face // 2
            at = jnp.broadcast_to(where_at[face : face + 1, :], (8, lanes))
            is_packed = odd == direction
            at_high = jnp.where(is_packed, jnp.minimum(at + half, lanes - 1), at)
            hops = jnp.broadcast_to(hop_of[face : face + 1, :], (8, lanes))
            for r in range(0, area, 8):
                row = slot * area + r
                if 0 in hops_in:
                    block = jnp.zeros((8, lanes), F32)
                else:
                    block = self.ghosts[face, pl.ds(r, 8), :]
                for hop in hops_in:
                    index = at
                    if hop == 0:
                        window = faces[direction, pl.ds(row, 8), :]
                    elif hop < HOPS or row < pack:
                        window = windows[direction, hop - 1, pl.ds(row, 8), :]
                    else:
                        start = pl.multiple_of(row - jnp.where(is_packed, pack, 0), 8)
                        window = windows[direction, hop - 1, pl.ds(start, 8), :]
                        index = at_high
                    block = jnp.where(hops == hop, pick(window, index), block)
                self.ghosts[face, pl.ds(r, 8), :] = block

        def near(self):
            for face in range(6):
                self.pull(face, (0,))

        def forward(self):
            self.relays = {}
            for direction, chunk, rows, made in self.links:
                comes = earlier_pair if direction == 0 else later_pair
                relay = send(
                    self.windows.at[direction, arrives[direction], rows],
                    self.windows.at[direction, 1, rows],
                    relay_sems,
                    (self.stage, direction, chunk),
                    partner,
                    comes,
                )

                @pl.when(comes)
                def _():
                    made.wait_recv()
                    relay.start()

                self.relays[direction, chunk] = (relay, comes)

        def collect(self):
            self.inside.wait_recv()
            pl.when(far_there)(self.far.wait_recv)
            for face in range(6):
                waits = self.relays.pop((face % 2, face // 2), None)
                if waits is not None:
                    relay, comes = waits
                    pl.when(comes)(relay.wait_recv)
                self.pull(face, (1, 2, 3))

    class Direct(Exchange):
        def post(self):
            faces, packed, windows, stage = self.faces, self.packed, self.windows, self.stage
            pack = 3 * self.area // 2
            self.links = []

            def start(hop, direction, src, dst):
                target = me + hop if direction == 0 else me - hop
                source_at = me - hop if direction == 0 else me + hop
                there = (target >= 0) & (target < total)
                comes = (source_at >= 0) & (source_at < total)
                at = (stage, direction, hop - 1)
                made = send(src, dst, link_sems, at, (target + total) % total, there)
                pl.when(there)(made.start)
                self.links.append((made, comes))

            for hop in (3, 2, 1):
                for direction in (0, 1):
                    if hop < HOPS:
                        start(hop, direction, faces.at[direction], windows.at[direction, hop - 1])
                        continue
                    index = last_index if direction == 0 else near_index
                    for r in range(0, pack, 8):
                        a = pick(faces[direction, pl.ds(r, 8), :], index)
                        b = pick(faces[direction, pl.ds(pack + r, 8), :], index)
                        packed[direction, pl.ds(r, 8), :] = jnp.where(low_half, a, b)
                    start(
                        hop,
                        direction,
                        packed.at[direction],
                        windows.at[direction, hop - 1, pl.ds(0, pack)],
                    )

        def pull(self, face, hops_in):
            area, faces, windows = self.area, self.faces, self.windows
            pack = 3 * area // 2
            direction, slot = face % 2, face // 2
            at = jnp.broadcast_to(where_direct[face : face + 1, :], (8, lanes))
            at_high = jnp.minimum(at + half, lanes - 1)
            hops = jnp.broadcast_to(hop_of[face : face + 1, :], (8, lanes))
            for r in range(0, area, 8):
                row = slot * area + r
                if 0 in hops_in:
                    block = jnp.zeros((8, lanes), F32)
                else:
                    block = self.ghosts[face, pl.ds(r, 8), :]
                for hop in hops_in:
                    if hop == 0:
                        moved = pick(faces[direction, pl.ds(row, 8), :], at)
                    elif hop < HOPS:
                        moved = pick(windows[direction, hop - 1, pl.ds(row, 8), :], at)
                    else:
                        window = windows[direction, hop - 1, pl.ds(row % pack, 8), :]
                        moved = pick(window, at if row < pack else at_high)
                    block = jnp.where(hops == hop, moved, block)
                self.ghosts[face, pl.ds(r, 8), :] = block

        def forward(self):
            pass

        def collect(self):
            for made, comes in self.links:
                pl.when(comes)(made.wait_recv)
            for face in range(6):
                self.pull(face, (1, 2, 3))

    def fine_exchange(k):
        return Exchange(
            k, 64, 3, faces_fine.at[k], packed_fine.at[k], windows_fine.at[k], ghosts_fine.at[k]
        )

    def coarse_exchange(k):
        kind = Direct if k in (1, 3) else Exchange
        packed = packed_coarse.at[k]
        return kind(
            3 + k,
            16,
            1,
            faces_coarse.at[k],
            packed if k in (1, 3) else packed.at[0],
            windows_coarse.at[k],
            ghosts_coarse.at[k],
        )

    zrow = lax.broadcasted_iota(jnp.int32, (8, 8, lanes), 1)

    def inner(values):
        for x in range(8):
            rows = pl.ds(64 * x, 64)
            here = values[rows, :]
            edge = jnp.zeros((8, lanes), F32)
            beside = jnp.concatenate([edge, here[:-8]], axis=0) + jnp.concatenate(
                [here[8:], edge], axis=0
            )
            if x > 0:
                beside = beside + values[pl.ds(64 * (x - 1), 64), :]
            if x < 7:
                beside = beside + values[pl.ds(64 * (x + 1), 64), :]
            cube = here.reshape(8, 8, lanes)
            below = jnp.where(zrow == 0, 0.0, pltpu.roll(cube, 1, 1))
            above = jnp.where(zrow == 7, 0.0, pltpu.roll(cube, 7, 1))
            beside = beside + (below + above).reshape(64, lanes)
            applied_ref[rows, :] = 6.0 * here - beside

    def with_ghosts(ghost, use):
        zghost[pl.ds(0, 64, 8), :] = ghost(4, 0, 64)
        zghost[pl.ds(7, 64, 8), :] = ghost(5, 0, 64)
        for x in range(8):
            rows = pl.ds(64 * x, 64)
            outer = zghost[rows, :]
            if x == 0:
                outer = outer + ghost(0, 0, 64)
            if x == 7:
                outer = outer + ghost(1, 0, 64)
            outer = jnp.concatenate(
                [
                    outer[:8] + ghost(2, 8 * x, 8),
                    outer[8:56],
                    outer[56:] + ghost(3, 8 * x, 8),
                ],
                axis=0,
            )
            use(x, rows, outer)

    def stored(ghosts):
        return lambda face, start, size: ghosts[face, pl.ds(start, size), :]

    def prolonged(k):
        def ghost(face, start, size):
            return jnp.concatenate(
                [
                    doubled[k, face, pl.ds(8 * (a // 2), 8), :]
                    for a in range(start // 8, (start + size) // 8)
                ],
                axis=0,
            )

        return ghost

    def double(k, face, value):
        doubled[k, face, pl.ds(0, 16, 2), :] = value
        doubled[k, face, pl.ds(1, 16, 2), :] = value

    def coarse_outer(ghosts):
        zghost_coarse[pl.ds(0, 16, 4), :] = ghosts[4]
        zghost_coarse[pl.ds(3, 16, 4), :] = ghosts[5]
        for x in range(4):
            yghost_coarse[pl.ds(16 * x, 4), :] = ghosts[2, pl.ds(4 * x, 4), :]
            yghost_coarse[pl.ds(16 * x + 12, 4), :] = ghosts[3, pl.ds(4 * x, 4), :]
        outer = yghost_coarse[...] + zghost_coarse[...]
        return jnp.concatenate(
            [outer[:16] + ghosts[0], outer[16:48], outer[48:] + ghosts[1]], axis=0
        )

    exchange = fine_exchange(0)
    cut(first, 8, exchange.faces)
    pl.semaphore_wait(barrier, greeted)
    exchange.post()
    pass_word(1)
    exchange.near()
    inner(first)
    exchange.forward()
    pass_word(2)
    exchange.collect()

    def sweep(x, rows, outer):
        second[rows, :] = first[rows, :] + RELAX_FINE * (
            source[rows, :] - applied_ref[rows, :] + outer
        )

    with_ghosts(stored(exchange.ghosts), sweep)

    smoothed = fine_exchange(1)
    sampled = coarse_exchange(0)
    cut(second, 8, smoothed.faces)
    for direction in (0, 1):
        for k in range(12):
            halved[direction, pl.ds(8 * k, 8), :] = (
                smoothed.faces[direction, pl.ds(16 * k, 8), :]
                + smoothed.faces[direction, pl.ds(16 * k + 8, 8), :]
            )
        sampled.faces[direction, :, :] = (
            halved[direction, pl.ds(0, 48, 2), :] + halved[direction, pl.ds(1, 48, 2), :]
        )
    sampled.post()
    smoothed.post()
    sampled.near()
    inner(second)
    for x in range(0, 8, 2):
        lower, upper = pl.ds(64 * x, 64), pl.ds(64 * x + 64, 64)
        both = (source[lower, :] - applied_ref[lower, :]) + (
            source[upper, :] - applied_ref[upper, :]
        )
        for y in range(4):
            paired[pl.ds(32 * (x // 2) + 8 * y, 8), :] = (
                both[16 * y : 16 * y + 8] + both[16 * y + 8 : 16 * y + 16]
            )
    inner_rhs = paired[pl.ds(0, 64, 2), :] + paired[pl.ds(1, 64, 2), :]
    smoothed.near()
    sampled.forward()
    pass_word(3)
    sampled.collect()
    coarse_rhs = 0.125 * (inner_rhs + coarse_outer(sampled.ghosts))
    coarse_one = RELAX_COARSE * coarse_rhs

    exchange = coarse_exchange(1)
    coarse = halved.at[0]
    coarse[0:64, :] = coarse_one
    cut(coarse, 4, exchange.faces)
    exchange.post()
    exchange.near()
    row = lax.broadcasted_iota(jnp.int32, (64, lanes), 0)
    edge = jnp.zeros((16, lanes), F32)
    beside = jnp.concatenate([edge, coarse_one[:-16]], axis=0) + jnp.concatenate(
        [coarse_one[16:], edge], axis=0
    )
    beside = beside + jnp.where(row // 4 % 4 == 0, 0.0, pltpu.roll(coarse_one, 4, 0))
    beside = beside + jnp.where(row // 4 % 4 == 3, 0.0, pltpu.roll(coarse_one, 60, 0))
    beside = beside + jnp.where(row % 4 == 0, 0.0, pltpu.roll(coarse_one, 1, 0))
    beside = beside + jnp.where(row % 4 == 3, 0.0, pltpu.roll(coarse_one, 63, 0))
    coarse_two = coarse_one + RELAX_COARSE * (coarse_rhs - 0.25 * (6.0 * coarse_one - beside))
    smoothed.forward()
    exchange.forward()
    for step in range(4, total // group_size + 1):
        pass_word(step)
    exchange.collect()
    coarse_two = coarse_two + (0.25 * RELAX_COARSE) * coarse_outer(exchange.ghosts)

    corrected = coarse_exchange(2)
    coarse[0:64, :] = coarse_two
    cut(coarse, 4, corrected.faces)
    corrected.post()
    paired[pl.ds(0, 64, 2), :] = coarse_two
    paired[pl.ds(1, 64, 2), :] = coarse_two
    for x in range(8):
        for y in range(8):
            rows = pl.ds(64 * x + 8 * y, 8)
            lift = paired[pl.ds(32 * (x // 2) + 8 * (y // 2), 8), :]
            second[rows, :] = second[rows, :] + lift
    inner(second)
    smoothed.collect()

    def smooth(x, rows, outer):
        first[rows, :] = second[rows, :] + RELAX_FINE * (
            source[rows, :] - applied_ref[rows, :] + outer
        )

    with_ghosts(stored(smoothed.ghosts), smooth)
    almost = fine_exchange(2)
    cut(first, 8, almost.faces)
    almost.post()
    corrected.near()
    corrected.forward()
    corrected.collect()

    edges = coarse_exchange(3)
    for direction in (0, 1):
        at = 3 if direction == 0 else 0
        along_rows, across_rows = pl.ds(4 * at, 4), pl.ds(at, 4, 4)
        lines = [(g, along_rows) for g in (2, 3, 4, 5)]
        lines += [(g, along_rows) for g in (0, 1)] + [(g, across_rows) for g in (4, 5)]
        lines += [(g, across_rows) for g in (0, 1, 2, 3)]
        for k, (g, rows) in enumerate(lines):
            edges.faces[direction, pl.ds(4 * k, 4), :] = corrected.ghosts[g, rows, :]
    edges.post()
    edges.near()
    for face in range(6):
        double(0, face, corrected.ghosts[face])
        own = corrected.faces[1 - face % 2, pl.ds(16 * (face // 2), 16), :]
        double(1, face, jnp.where(hop_of[face : face + 1, :] >= 0, own, 0.0))

    def lift(x, rows, outer):
        first[rows, :] = first[rows, :] + RELAX_FINE * outer

    with_ghosts(prolonged(0), lift)
    inner(first)
    almost.near()
    almost.forward()
    almost.collect()
    outermost = almost.ghosts
    own = prolonged(1)
    for face in range(6):
        outermost[face] = outermost[face] + RELAX_FINE * own(face, 0, 64)
    edges.forward()
    edges.collect()
    for face in range(6):
        double(0, face, RELAX_FINE * edges.ghosts[face])
        for k, rows in enumerate((pl.ds(0, 8), pl.ds(56, 8), pl.ds(0, 8, 8), pl.ds(7, 8, 8))):
            outermost[face, rows, :] = (
                outermost[face, rows, :] + doubled[0, face, pl.ds(8 * k, 8), :]
            )

    parts = [jnp.zeros((8, lanes), F32)] * 5

    def fold(block):
        return jnp.sum(block.reshape(8, 8, lanes), axis=0)

    def close(x, rows, outer):
        here = first[rows, :]
        applied = applied_ref[rows, :] - outer
        image[rows, :] = applied
        r = source[rows, :]
        for k, term in enumerate((r * here, here * applied, r * r, r * applied, applied * applied)):
            parts[k] = parts[k] + fold(term)

    with_ghosts(stored(outermost), close)

    tile = jnp.zeros((1, lanes), F32)
    for k in range(5):
        one = jnp.sum(jnp.sum(parts[k], axis=0, keepdims=True), axis=1, keepdims=True)
        tile = jnp.where(lane == k, one, tile)
    base = 0
    for stage, (size, mine, peer) in enumerate(stages):
        sums[base + mine] = tile
        for k in range(1, size):
            made = pltpu.make_async_remote_copy(
                src_ref=sums.at[base + mine],
                dst_ref=sums.at[base + mine],
                send_sem=sum_send.at[stage],
                recv_sem=sum_recv.at[stage],
                device_id=peer(k),
                device_id_type=MESH,
            )
            made.start()
        arriving = sums.at[pl.ds(base, size - 1)]
        for made, sends in finishing:
            if sends is None:
                made.wait_send()
            else:
                pl.when(sends)(made.wait_send)
        finishing.clear()
        pltpu.make_async_copy(arriving, arriving, sum_send.at[stage]).wait()
        pltpu.make_async_copy(arriving, arriving, sum_recv.at[stage]).wait()
        tile = jnp.sum(sums[base : base + size], axis=0)
        base += size
    tile_ref[...] = tile


def finish(p_ref, image_ref, source_ref, tile_ref, sol_hbm, res_hbm, norm_ref, sol, res, sems):
    lanes = p_ref.shape[1]
    rows_per = p_ref.shape[0] // PIECES
    lane = lax.broadcasted_iota(jnp.int32, (1, lanes), 1)
    tile = tile_ref[...]
    along, curvature, old_square, cross, image_square = [
        jnp.sum(jnp.where(lane == k, tile, 0.0), axis=1, keepdims=True) for k in range(5)
    ]
    step = along / curvature
    copies = []
    for x in range(PIECES):
        rows = pl.ds(rows_per * x, rows_per)
        sol[rows, :] = step * p_ref[rows, :]
        res[rows, :] = source_ref[rows, :] - step * image_ref[rows, :]
        for k, (here, there) in enumerate(((sol, sol_hbm), (res, res_hbm))):
            made = pltpu.make_async_copy(here.at[rows], there.at[rows], sems.at[k, x])
            made.start()
            copies.append(made)
    square = old_square - 2.0 * step * cross + step * step * image_square
    norm_ref[0] = jnp.sqrt(square)[0, 0]
    for made in copies:
        made.wait()


def local(sizes, right_side, counts, neighbours):
    cells, lanes = right_side.shape
    curve_size, level_size = sizes
    total = curve_size * level_size
    group_size = level_size * (2 - curve_size % 2)

    def body(*refs):
        curve, level = lax.axis_index("curve"), lax.axis_index("level")
        if total <= 64:
            me = curve * level_size + level

            def everyone(k):
                other = (me + k) % total
                return (other // level_size, other % level_size)

            stages = [(total, me, everyone)]
        else:
            stages = [
                (level_size, level, lambda k: (curve, (level + k) % level_size)),
                (curve_size, curve, lambda k: ((curve + k) % curve_size, level)),
            ]
        kernel(sizes, stages, group_size, *refs)

    sum_rows = total if total <= 64 else curve_size + level_size
    vmem = pl.BlockSpec(memory_space=pltpu.VMEM)
    block = jax.ShapeDtypeStruct((cells, lanes), F32)
    whole = pltpu.VMEM((cells, lanes), F32)
    out = pl.pallas_call(
        body,
        out_shape=(whole, whole, whole, pltpu.VMEM((1, lanes), F32)),
        in_specs=[pl.BlockSpec(memory_space=pl.ANY)] * 3,
        out_specs=(vmem,) * 4,
        scratch_shapes=[
            pltpu.SMEM(counts.shape, jnp.int32),
            pltpu.VMEM(neighbours.shape, jnp.int32),
            pltpu.VMEM((cells, lanes), F32),
            pltpu.VMEM((cells, lanes), F32),
            pltpu.VMEM((cells // 4, lanes), F32),
            pltpu.VMEM((2, 96, lanes), F32),
            pltpu.VMEM((cells // 8, lanes), F32),
            pltpu.VMEM((cells // 8, lanes), F32),
            pltpu.VMEM((2, 6, 32, lanes), F32),
            pltpu.VMEM((cells, lanes), F32),
            pltpu.VMEM((3, 6, 64, lanes), F32),
            pltpu.VMEM((4, 6, 16, lanes), F32),
            pltpu.VMEM((3, 2, 192, lanes), F32),
            pltpu.VMEM((3, 96, lanes), F32),
            pltpu.VMEM((3, 2, HOPS, 192, lanes), F32),
            pltpu.VMEM((4, 2, 48, lanes), F32),
            pltpu.VMEM((4, 2, 24, lanes), F32),
            pltpu.VMEM((4, 2, HOPS, 48, lanes), F32),
            pltpu.VMEM((sum_rows, 1, lanes), F32),
            pltpu.SemaphoreType.DMA((3,)),
            pltpu.SemaphoreType.REGULAR((2, max(1, total // group_size - 1))),
            pltpu.SemaphoreType.DMA((7, 2, 3)),
            pltpu.SemaphoreType.DMA((7, 2, 3)),
            pltpu.SemaphoreType.DMA((7, 2, 3)),
            pltpu.SemaphoreType.DMA((7, 2, 3)),
            pltpu.SemaphoreType.DMA((7,)),
            pltpu.SemaphoreType.DMA((7,)),
            pltpu.SemaphoreType.DMA((7,)),
            pltpu.SemaphoreType.DMA((7,)),
            pltpu.SemaphoreType.DMA((2,)),
            pltpu.SemaphoreType.DMA((2,)),
        ],
        compiler_params=pltpu.CompilerParams(collective_id=0, has_side_effects=True),
    )(right_side, counts, neighbours)
    hbm = pl.BlockSpec(memory_space=pl.ANY)
    out = pl.pallas_call(
        finish,
        out_shape=(block, block, jax.ShapeDtypeStruct((1,), F32)),
        in_specs=[vmem] * 4,
        out_specs=(hbm, hbm, pl.BlockSpec(memory_space=pltpu.SMEM)),
        scratch_shapes=[
            pltpu.VMEM((cells, lanes), F32),
            pltpu.VMEM((cells, lanes), F32),
            pltpu.SemaphoreType.DMA((2, PIECES)),
        ],
    )(*[pltpu.with_memory_space_constraint(a, pltpu.VMEM) for a in out])
    return out[0], out[1], out[2].reshape(())


def solution(mesh):
    sizes = tuple(mesh.shape[name] for name in AXES)
    in_specs = (P(None, AXES), P(), P(None, AXES))
    out_specs = (P(None, AXES), P(None, AXES), P())
    return jax.shard_map(
        functools.partial(local, sizes), mesh=mesh, in_specs=in_specs, out_specs=out_specs, check_vma=False
    )
```
